128 devices in a mesh: section: 4 (over x), fsdp: 32 (over y, z, core).
Axes of the slice: x: 4, y: 4, z: 4, core: 2. Of those that a mesh axis runs over, the one named last changes fastest.
Arguments:
- grad_parts: bfloat16 [4, 32, 8192, 1024], P('section', 'fsdp'), may hold values from -510 to 510
- first_codes: int32 [4, 8192, 1024], P('section', 'fsdp'), may hold values from -7 to 7
- first_rows: float32 [4, 8192], P('section', 'fsdp'), may hold values from 0.003 to 0.03
- first_columns: float32 [4, 1024], P('section'), may hold values from 0.003 to 0.03
- second_codes: int32 [4, 8192, 1024], P('section', 'fsdp'), may hold values from 1 to 15
- second_rows: float32 [4, 8192], P('section', 'fsdp'), may hold values from 0.001 to 0.01
- second_columns: float32 [4, 1024], P('section'), may hold values from 0.001 to 0.01
Outputs:
- direction: float32 [4, 8192, 1024], P('section', 'fsdp')
- first_scaled: float32 [4, 8192, 1024], P('section', 'fsdp')
- second_scaled: float32 [4, 8192, 1024], P('section', 'fsdp')
- first_rowmax: float32 [4, 8192], P('section', 'fsdp')
- first_colmax: float32 [4, 1024], P('section')
- second_rowmax: float32 [4, 8192], P('section', 'fsdp')
- second_colmax: float32 [4, 1024], P('section')
The draws below stay inside these ranges and needn't reach their ends.
All inputs are finite; a program needn't handle non-finite values. Where the reference program divides by a largest or mean magnitude, that divisor is 1e-20 or more.
Results may differ from the reference program's by a relative error of at most 0.0003.
Values may be sent and summed in bfloat16 or wider, within the bound.
No kernel may reach another device: no remote copies, remote signals or barrier semaphores. Data moves between devices by JAX's collectives and lax.ppermute only.
A program may use at most 192 MiB of HBM per device.

```python
import math
import jax
import jax.numpy as jnp
from jax import lax

ROWS = 8192
KV = 1024
LAYERS_ALL = 4
PARTIALS = 32


def draw_grad_parts(key, part):
    subkeys = jax.random.split(key, 5)
    full_shape = (LAYERS_ALL, PARTIALS, ROWS, KV)
    col_scale = jnp.exp(jax.random.uniform(subkeys[0], (LAYERS_ALL, 1, 1, KV), jnp.float32, math.log(0.2), math.log(5.0)))
    row_scale = jnp.exp(jax.random.uniform(subkeys[1], (LAYERS_ALL, 1, ROWS, 1), jnp.float32, math.log(0.5), math.log(2.0)))
    owner_block = jax.random.randint(subkeys[2], (LAYERS_ALL, PARTIALS, 1, 1), 0, PARTIALS)
    row_block = (jnp.arange(ROWS, dtype=jnp.int32) // (ROWS // PARTIALS)).reshape(1, 1, ROWS, 1)
    spike_gain = jnp.where(row_block == owner_block, 4.0, 1.0)
    basis_values = jnp.clip(jax.random.normal(subkeys[3], full_shape, jnp.float32), -6.0, 6.0)
    return (basis_values * col_scale * row_scale * spike_gain).astype(jnp.bfloat16)


def plant(result, key, least, high):
    longest = result.shape.index(max(result.shape))
    spots = []
    for shift in (0, 1):
        where = [jax.random.randint(jax.random.fold_in(key, axis), (), 0, length) for axis, length in enumerate(result.shape)]
        where[longest] = (where[longest] + shift) % result.shape[longest]
        spots.append(tuple(where))
    return result.at[spots[0]].set(least).at[spots[1]].set(high)


def shard_levels(rng, extent, cuts, least, largest):
    factor_of = 1.0
    for position, shards_of in cuts:
        heights = jax.random.uniform(jax.random.fold_in(jax.random.fold_in(rng, 6), position), (shards_of,), jnp.float32, least / len(cuts), largest / len(cuts))
        factor_of = factor_of * jnp.repeat(jnp.exp(heights), extent[position] // shards_of).reshape((-1,) + (1,) * (len(extent) - 1 - position))
    return factor_of


def setup_inputs(seed: int = 0) -> dict:
    keys = jax.random.split(jax.random.key(seed), 8)
    return {
        "grad_parts": draw_grad_parts(jax.random.fold_in(keys[7], 71), 0),
        "first_codes": plant(jax.random.randint(keys[1], (LAYERS_ALL, ROWS, KV), -7, 8), jax.random.fold_in(keys[1], 1), -7, 7).astype(jnp.int32),
        "first_rows": jnp.clip(jnp.exp(math.log(0.03) - 2.3025851 * jax.random.uniform(keys[2], (LAYERS_ALL, ROWS), jnp.float32) ** shard_levels(keys[2], (LAYERS_ALL, ROWS), ((0, 4), (1, 32)), -0.2, 0.2)), 0.003, 0.03),
        "first_columns": jnp.clip(jnp.exp(math.log(0.03) - 2.3025851 * jax.random.uniform(keys[3], (LAYERS_ALL, KV), jnp.float32) ** shard_levels(keys[3], (LAYERS_ALL, KV), ((0, 4),), -0.2, 0.2)), 0.003, 0.03),
        "second_codes": plant(jax.random.randint(keys[4], (LAYERS_ALL, ROWS, KV), 1, 16), jax.random.fold_in(keys[4], 1), 1, 15).astype(jnp.int32),
        "second_rows": jnp.clip(jnp.exp(math.log(0.01) - 2.30258502 * jax.random.uniform(keys[5], (LAYERS_ALL, ROWS), jnp.float32) ** shard_levels(keys[5], (LAYERS_ALL, ROWS), ((0, 4), (1, 32)), -0.2, 0.2)), 0.001, 0.01),
        "second_columns": jnp.clip(jnp.exp(math.log(0.01) - 2.30258502 * jax.random.uniform(keys[6], (LAYERS_ALL, KV), jnp.float32) ** shard_levels(keys[6], (LAYERS_ALL, KV), ((0, 4),), -0.2, 0.2)), 0.001, 0.01),
    }


beta_first = 0.9
beta_second = 0.999
clip_rms = 3.0
epsilon = 1e-08
scale_floor = 0.001

def dequantize(code_values, levels, row_scale, col_scale):
    scale_bound = jnp.minimum(row_scale[:, :, None], col_scale[:, None, :])
    return code_values.astype(jnp.float32) / levels * scale_bound

def moments(gradient, clip_scale, first_codes, first_rows, first_columns, second_codes, second_rows, second_columns):
    first_old = dequantize(first_codes, 7.0, first_rows, first_columns)
    second_old = dequantize(second_codes, 15.0, second_rows, second_columns)
    clipped = clip_scale * gradient
    first_new = beta_first * first_old + (1.0 - beta_first) * clipped
    second_new = beta_second * second_old + (1.0 - beta_second) * clipped * clipped
    direction = first_new / (jnp.sqrt(second_new) + epsilon)
    return (first_new, second_new, direction)

def reference(grad_parts, first_codes, first_rows, first_columns, second_codes, second_rows, second_columns):

    def add_part(which_part, running):
        partial_value = lax.dynamic_index_in_dim(grad_parts, which_part, 1, keepdims=False)
        return running + partial_value.astype(jnp.float32)
    gradient = lax.fori_loop(0, PARTIALS, add_part, jnp.zeros((LAYERS_ALL, ROWS, KV), jnp.float32))
    square_sum = jnp.sum(gradient * gradient)
    clip_limit = clip_rms * math.sqrt(LAYERS_ALL * ROWS * KV)
    clip_scale = clip_limit / jnp.maximum(jnp.sqrt(square_sum), clip_limit)
    first_new, second_new, direction = moments(gradient, clip_scale, first_codes, first_rows, first_columns, second_codes, second_rows, second_columns)
    first_rowmax = jnp.maximum(lax.optimization_barrier(jnp.max(jnp.abs(first_new), axis=2)), scale_floor)
    first_colmax = jnp.maximum(lax.optimization_barrier(jnp.max(jnp.abs(first_new), axis=1)), scale_floor)
    second_rowmax = lax.optimization_barrier(jnp.max(second_new, axis=2))
    second_colmax = lax.optimization_barrier(jnp.max(second_new, axis=1))
    first_scaled = first_new / jnp.minimum(first_rowmax[:, :, None], first_colmax[:, None, :])
    second_scaled = second_new / jnp.minimum(second_rowmax[:, :, None], second_colmax[:, None, :])
    return (direction, first_scaled, second_scaled, first_rowmax, first_colmax, second_rowmax, second_colmax)
```

```python
import functools
import math

import jax
import jax.numpy as jnp
from jax import lax
from jax.experimental import pallas as pl
from jax.experimental.pallas import tpu as pltpu
from jax.sharding import Mesh
from jax.sharding import PartitionSpec as P

AXES = ("section", "y", "z", "core")
FSDP = ("y", "z", "core")

beta_first = 0.9
beta_second = 0.999
clip_rms = 3.0
epsilon = 1e-08
scale_floor = 0.001

RING = 4
TOP = 32767.0
LEAST = 1e-18
F32, BF16, I16 = jnp.float32, jnp.bfloat16, jnp.int16


def scale_code(peak):
    return jnp.ceil(jnp.log2(jnp.maximum(peak, LEAST)) * 256.0)


def encode(values, code):
    factor = jnp.exp2(code * (-1.0 / 256.0)) * TOP**4
    root = lax.rsqrt(lax.rsqrt(jnp.maximum(jnp.abs(values) * factor, 1e-8)))
    root = jnp.where(values < 0.0, -root, root)
    return jnp.round(root).astype(jnp.int32).astype(I16)


def decode(codes, code):
    factor = jnp.exp2(code * (1.0 / 256.0)) * TOP**-4
    root = codes.astype(jnp.int32).astype(F32)
    return (root * jnp.abs(root)) * (root * root) * factor


def block_of(half, delta, j, where):
    if half == 0:
        return lax.rem(where[0] + delta, RING) * RING + j
    return j * RING + lax.rem(where[1] + delta, RING)


def cost(flops, bytes_accessed):
    return pl.CostEstimate(flops=flops, bytes_accessed=bytes_accessed, transcendentals=0)


def gather_body(where, first, second, out):
    out[0, 0] = first[0, 0, 0]
    out[1, 0] = second[0, 0, 0]


def part_spec(half, delta, mine, rows, cols):
    def index(j, where):
        core = where[2] if mine else 1 - where[2]
        return block_of(half, delta, j, where), core, half, 0, 0

    return pl.BlockSpec((1, 1, 1, rows, cols), index)


def gather(where, parts, jobs):
    rows, cols = parts.shape[3:]
    return pl.pallas_call(
        gather_body,
        out_shape=jax.ShapeDtypeStruct((2, RING, rows, cols), parts.dtype),
        grid_spec=pltpu.PrefetchScalarGridSpec(
            num_scalar_prefetch=1,
            grid=(RING,),
            in_specs=[part_spec(h, d, False, rows, cols) for h, d in jobs],
            out_specs=pl.BlockSpec((2, 1, rows, cols), lambda j, where: (0, j, 0, 0)),
        ),
        cost_estimate=cost(2 * RING * rows * cols, 16 * RING * rows * cols),
        name="gather",
    )(where, parts, parts)


def pair_body(where, first, second, came, out_first, out_second):
    j = pl.program_id(0)
    rows = first.shape[3]
    for own, k, out in ((first, 0, out_first), (second, 1, out_second)):
        total = own[0, 0, 0].astype(F32) + came[k, 0].astype(F32)
        code = scale_code(jnp.max(jnp.abs(total), axis=0, keepdims=True))
        out[pl.ds(pl.multiple_of(j * rows, rows), rows), :] = encode(total, code)
        at = RING * rows
        side = out[at : at + 16, :].astype(jnp.int32).astype(F32)
        line = lax.broadcasted_iota(jnp.int32, side.shape, 0)
        side = jnp.where(line == j, code, jnp.where(line < j, side, 0.0))
        out[at : at + 16, :] = side.astype(jnp.int32).astype(I16)


def pair(where, parts, came, jobs):
    rows, cols = parts.shape[3:]
    sent = jax.ShapeDtypeStruct((RING * rows + 16, cols), I16)
    whole = pl.BlockSpec(sent.shape, lambda j, where: (0, 0))
    return pl.pallas_call(
        pair_body,
        out_shape=(sent, sent),
        grid_spec=pltpu.PrefetchScalarGridSpec(
            num_scalar_prefetch=1,
            grid=(RING,),
            in_specs=[part_spec(h, d, True, rows, cols) for h, d in jobs]
            + [pl.BlockSpec((2, 1, rows, cols), lambda j, where: (0, j, 0, 0))],
            out_specs=(whole, whole),
        ),
        cost_estimate=cost(60 * RING * rows * cols, 12 * RING * rows * cols),
        name="pair",
    )(where, parts, parts, came)


def middle_body(half, where, own, came, *refs):
    got, (out_next, out_last, out_far, kept) = refs[:6], refs[6:]
    k = pl.program_id(0)
    j = lax.rem(where[1 - half] + jnp.where(k == 0, 1, jnp.where(k == 1, 3, jnp.where(k == 2, 2, 0))), RING)
    rows = own.shape[3]
    total = own[0, 0, 0].astype(F32) + came[0, 0].astype(F32)
    line = lax.broadcasted_iota(jnp.int32, (16, own.shape[4]), 0)
    for codes, side in zip(got[:3], got[3:]):
        code = side[...].astype(jnp.int32).astype(F32)
        code = jnp.sum(jnp.where(line == j, code, 0.0), axis=0, keepdims=True)
        total = total + decode(codes[...], code)
    for at, out in enumerate((out_next, out_last, out_far)):

        @pl.when(k == at)
        def _(out=out):
            code = scale_code(jnp.max(jnp.abs(total), axis=0, keepdims=True))
            out[0:rows, :] = encode(total, code)
            out[rows : rows + 16, :] = jnp.broadcast_to(code.astype(jnp.int32), (16, code.shape[1])).astype(I16)

    @pl.when(k == 3)
    def _():
        kept[...] = total


def middle(where, parts, came, got, half):
    rows, cols = parts.shape[3:]

    def j_of(k, where):
        delta = jnp.where(k == 0, 1, jnp.where(k == 1, 3, jnp.where(k == 2, 2, 0)))
        return lax.rem(where[1 - half] + delta, RING)

    def own_index(k, where):
        return block_of(half, 0, j_of(k, where), where), where[2], half, 0, 0

    sent = jax.ShapeDtypeStruct((rows + 16, cols), I16)
    whole = pl.BlockSpec(sent.shape, lambda k, where: (0, 0))
    return pl.pallas_call(
        functools.partial(middle_body, half),
        out_shape=(sent, sent, sent, jax.ShapeDtypeStruct((rows, cols), F32)),
        grid_spec=pltpu.PrefetchScalarGridSpec(
            num_scalar_prefetch=1,
            grid=(RING,),
            in_specs=[
                pl.BlockSpec((1, 1, 1, rows, cols), own_index),
                pl.BlockSpec((1, 1, rows, cols), lambda k, where: (half, j_of(k, where), 0, 0)),
            ]
            + [pl.BlockSpec((rows, cols), lambda k, where: (j_of(k, where), 0))] * 3
            + [pl.BlockSpec((16, cols), lambda k, where: (RING * rows // 16, 0))] * 3,
            out_specs=(whole, whole, whole, pl.BlockSpec((rows, cols), lambda k, where: (0, 0))),
        ),
        cost_estimate=cost(60 * RING * rows * cols, 12 * RING * rows * cols),
        name="middle",
    )(where, parts, came, *got, *got)


def last_body(*refs):
    ins, (grad, squares) = refs[:8], refs[8:]
    rows = ins[0].shape[0]
    square = jnp.zeros((1, ins[0].shape[1]), F32)
    for half in range(2):
        kept, *got = ins[4 * half : 4 * half + 4]
        total = kept[...]
        for ref in got:
            code = ref[rows : rows + 16, :].astype(jnp.int32).astype(F32)[0:1]
            total = total + decode(ref[0:rows, :], code)
        grad[0, half * rows : (half + 1) * rows, :] = total
        square = square + jnp.sum(total * total, axis=0, keepdims=True)
    folded = square[:, 0:128]
    for at in range(128, square.shape[1], 128):
        folded = folded + square[:, at : at + 128]
    squares[...] = jnp.broadcast_to(folded, squares.shape)


def last(halves, devices):
    rows, cols = halves[0][0].shape
    flat = [a for half in halves for a in half]
    return pl.pallas_call(
        last_body,
        out_shape=(
            jax.ShapeDtypeStruct((1, 2 * rows, cols), F32),
            jax.ShapeDtypeStruct((devices, 128), F32),
        ),
        cost_estimate=cost(60 * rows * cols, 24 * rows * cols),
        name="last",
    )(*flat)


def reduce_scatter(parts, devices):
    where = jnp.stack([lax.axis_index(a) for a in FSDP]).astype(jnp.int32)
    axis = ("y", "z")

    def hop(value, name, delta):
        return lax.ppermute(value, name, [(i, (i + delta) % RING) for i in range(RING)])

    def swap(jobs):
        return lax.ppermute(gather(where, parts, jobs), "core", [(0, 1), (1, 0)])

    jobs = (((0, 1), (0, 3)), ((1, 1), (1, 3)), ((0, 2), (1, 2)), ((0, 0), (1, 0)))
    came = [swap(j) for j in jobs]
    sent = {}
    for j, c in zip(jobs[:3], came[:3]):
        for job, out in zip(j, pair(where, parts, c, j)):
            sent[job] = hop(out, axis[job[0]], job[1])
    halves = []
    for half in range(2):
        got = [sent[half, d] for d in (1, 3, 2)]
        *out, kept = middle(where, parts, came[3], got, half)
        halves.append([kept] + [hop(o, axis[1 - half], d) for o, d in zip(out, (1, 3, 2))])
    return last(halves, devices)


def copy_for_each(value, axis):
    copies = jnp.broadcast_to(value, (lax.axis_size(axis), *value.shape))
    return lax.all_to_all(copies, axis, split_axis=0, concat_axis=0, tiled=True)


def of_everyone(value, axis):
    everything = copy_for_each(value, axis)
    return jnp.max(everything, axis=0)


def in_one(arrays, axis):
    flat, at, outs = (jnp.concatenate([a.reshape(-1) for a in arrays]), 0, [])
    total = of_everyone(flat, axis)
    for a in arrays:
        outs.append(total[at : at + a.size].reshape(a.shape))
        at += a.size
    return tuple(outs)


def dequantize(code_values, levels, row_scale, col_scale):
    scale_bound = jnp.minimum(row_scale[:, :, None], col_scale[:, None, :])
    return code_values.astype(jnp.float32) / levels * scale_bound


def moments(
    gradient,
    clip_scale,
    first_codes,
    first_rows,
    first_columns,
    second_codes,
    second_rows,
    second_columns,
):
    first_old = dequantize(first_codes, 7.0, first_rows, first_columns)
    second_old = dequantize(second_codes, 15.0, second_rows, second_columns)
    clipped = clip_scale * gradient
    first_new = beta_first * first_old + (1.0 - beta_first) * clipped
    second_new = beta_second * second_old + (1.0 - beta_second) * clipped * clipped
    direction = first_new / (jnp.sqrt(second_new) + epsilon)
    return (first_new, second_new, direction)


def local(
    grad_parts, first_codes, first_rows, first_columns, second_codes, second_rows, second_columns
):
    layer_count, _, row_count, col_count = grad_parts.shape
    entries = layer_count * lax.axis_size("section") * row_count * col_count
    devices = lax.axis_size(AXES)
    parts = grad_parts.reshape(RING * RING, 2, 2, -1, col_count)
    gradient, squares = reduce_scatter(parts, devices)
    squares = lax.all_to_all(squares, AXES, split_axis=0, concat_axis=0, tiled=True)
    square_sum = jnp.sum(squares)
    clip_limit = clip_rms * math.sqrt(entries)
    clip_scale = clip_limit / jnp.maximum(jnp.sqrt(square_sum), clip_limit)
    first_new, second_new, direction = moments(
        gradient,
        clip_scale,
        first_codes,
        first_rows,
        first_columns,
        second_codes,
        second_rows,
        second_columns,
    )
    first_rowmax = jnp.maximum(jnp.max(jnp.abs(first_new), axis=2), scale_floor)
    first_local = jnp.max(jnp.abs(first_new), axis=1)
    second_rowmax = jnp.max(second_new, axis=2)
    second_local = jnp.max(second_new, axis=1)
    first_colmax, second_colmax = in_one((first_local, second_local), FSDP)
    first_colmax = jnp.maximum(first_colmax, scale_floor)
    first_scaled = first_new / jnp.minimum(first_rowmax[:, :, None], first_colmax[:, None, :])
    second_scaled = second_new / jnp.minimum(second_rowmax[:, :, None], second_colmax[:, None, :])
    return (
        direction,
        first_scaled,
        second_scaled,
        first_rowmax,
        first_colmax,
        second_rowmax,
        second_colmax,
    )


def solution(mesh):
    torus = Mesh(mesh.devices.reshape(mesh.shape["section"], RING, RING, 2), AXES)
    placed = (
        P("section", FSDP, None, None),
        P("section", FSDP, None),
        P("section", FSDP),
        P("section", None),
        P("section", FSDP, None),
        P("section", FSDP),
        P("section", None),
    )
    return jax.shard_map(
        local,
        mesh=torus,
        in_specs=placed,
        out_specs=(
            P("section", FSDP, None),
            P("section", FSDP, None),
            P("section", FSDP, None),
            P("section", FSDP),
            P("section", None),
            P("section", FSDP),
            P("section", None),
        ),
        check_vma=False,
    )
```

```python
import functools
import math

import jax
import jax.numpy as jnp
from jax import lax
from jax.experimental import pallas as pl
from jax.experimental.pallas import tpu as pltpu
from jax.sharding import Mesh
from jax.sharding import PartitionSpec as P

AXES = ("section", "y", "z", "core")
FSDP = ("y", "z", "core")

beta_first = 0.9
beta_second = 0.999
clip_rms = 3.0
epsilon = 1e-08
scale_floor = 0.001

RING = 4
ORDER = (1, 3, 2, 0)
TOP = 32767.0
LEAST = 1e-18
SIDE = 8
STEP = 16
VMEM_LIMIT = 20 * 1024 * 1024
F32, BF16, I16 = jnp.float32, jnp.bfloat16, jnp.int16
VMEM = pltpu.VMEM


def scale_code(peak):
    return jnp.ceil(jnp.log2(jnp.maximum(peak, LEAST)) * 256.0)


def send_factor(code):
    return jnp.exp2(code * (-1.0 / 256.0)) * TOP**4


def encode(values, factor):
    root = lax.rsqrt(lax.rsqrt(jnp.maximum(jnp.abs(values) * factor, 1e-8)))
    root = jnp.where(values < 0.0, -root, root)
    return jnp.round(root).astype(jnp.int32).astype(I16)


def came_factor(side):
    code = side[...].astype(jnp.int32).astype(F32)
    return jnp.exp2(code * (1.0 / 256.0)) * TOP**-4


def decode(codes, factor):
    root = codes.astype(jnp.int32).astype(F32)
    square = root * root
    return (jnp.where(root < 0.0, -square, square) * square) * factor


def side_rows(codes):
    line = lax.broadcasted_iota(jnp.int32, (SIDE, codes[0].shape[1]), 0)
    rows = codes[-1]
    for at, code in enumerate(codes[:-1]):
        rows = jnp.where(line == at, code, rows)
    return jnp.broadcast_to(rows, line.shape).astype(jnp.int32).astype(I16)


def call(body, name, outs, scratch, flops, bytes_accessed, where=False):
    return pl.pallas_call(
        body,
        out_shape=outs,
        in_specs=where,
        out_specs=tuple(pl.BlockSpec(memory_space=VMEM) for _ in outs),
        scratch_shapes=scratch,
        compiler_params=pltpu.CompilerParams(vmem_limit_bytes=VMEM_LIMIT),
        cost_estimate=pl.CostEstimate(flops=flops, bytes_accessed=bytes_accessed, transcendentals=0),
        name=name,
    )


def in_vmem(n):
    return [pl.BlockSpec(memory_space=VMEM)] * n


def held(value):
    return pltpu.with_memory_space_constraint(value, VMEM)


def gather_body(wanted, where, parts, *refs):
    outs, sem = refs[:-1], refs[-1]
    copies = []
    for (jobs, mine), out in zip(wanted, outs):
        core = where[2] if mine else 1 - where[2]
        for q, (half, delta, low) in enumerate(jobs):
            for i in range(2):
                j = lax.rem(where[1 - half] + ORDER[low + i], RING)
                far = lax.rem(where[half] + delta, RING)
                at = far * RING + j if half == 0 else j * RING + far
                copies.append(
                    pltpu.make_async_copy(
                        parts.at[at, core, half], out.at[q, i], sem.at[len(copies)]
                    )
                )
    for copy in copies:
        copy.start()
    for copy in copies:
        copy.wait()


def gather(where, parts, wanted):
    rows, cols = parts.shape[3:]
    return call(
        functools.partial(gather_body, wanted),
        "gather",
        tuple(VMEM((4, 2, rows, cols), parts.dtype) for _ in wanted),
        [pltpu.SemaphoreType.DMA((8 * len(wanted),))],
        8 * rows * cols,
        32 * len(wanted) * rows * cols,
        [pl.BlockSpec(memory_space=pltpu.SMEM), pl.BlockSpec(memory_space=pltpu.HBM)],
    )(where, pltpu.with_memory_space_constraint(parts, pltpu.HBM))


def chunks(rows, step, carry):
    return lax.fori_loop(0, rows // STEP, lambda n, c: step(pl.multiple_of(n * STEP, STEP), c), carry)


def send_blocks(total, outs, peaks, rows, each):
    code = scale_code(jnp.concatenate(peaks, axis=0))
    factor = send_factor(code)
    for q, out in enumerate(outs):
        for i in range(each):
            line = q * each + i
            by = factor[line : line + 1]

            def step(r, _, line=line, by=by, out=out, i=i):
                out[pl.ds(i * rows + r, STEP), :] = encode(total[line, pl.ds(r, STEP), :], by)

            chunks(rows, step, None)
        out[each * rows : each * rows + SIDE, :] = side_rows(
            [code[q * each + i : q * each + i + 1] for i in range(each)]
        )


def pair_body(own, came, *refs):
    relayed, outs, total = refs[:-5], refs[-5:-1], refs[-1]
    rows, cols = own.shape[2:]
    peaks = []
    for q in range(4):
        by = came_factor(relayed[q].at[2 * rows : 2 * rows + SIDE]) if relayed else None
        for i in range(2):

            def step(r, peak, q=q, i=i, by=by):
                value = own[q, i, pl.ds(r, STEP), :].astype(F32) + came[q, i, pl.ds(r, STEP), :].astype(F32)
                if relayed:
                    value = value + decode(relayed[q][pl.ds(i * rows + r, STEP), :], by[i : i + 1])
                total[2 * q + i, pl.ds(r, STEP), :] = value
                return jnp.maximum(peak, jnp.abs(value))

            peak = chunks(rows, step, jnp.zeros((STEP, cols), F32))
            peaks.append(jnp.max(peak, axis=0, keepdims=True))
    send_blocks(total, outs, peaks, rows, 2)


def pair(own, came, relayed=()):
    rows, cols = own.shape[2:]
    sent = VMEM((2 * rows + SIDE, cols), I16)
    return call(
        pair_body,
        "pair",
        (sent,) * 4,
        [VMEM((8, rows, cols), F32)],
        400 * rows * cols,
        48 * rows * cols,
        in_vmem(2 + len(relayed)),
    )(own, held(came), *[held(r) for r in relayed])


def keep_body(own, came, *refs):
    got, total = refs[:4], refs[4]
    rows = own.shape[2]
    for half in range(2):
        for i in range(RING):
            ref = got[2 * half + (1 if i < 2 else 0)]
            by = came_factor(ref.at[2 * rows : 2 * rows + SIDE])[i % 2 : i % 2 + 1]

            def step(r, _, ref=ref, by=by, half=half, i=i):
                q = 2 * half + i // 2
                value = own[q, i % 2, pl.ds(r, STEP), :].astype(F32) + came[q, i % 2, pl.ds(r, STEP), :].astype(F32)
                total[half, i, pl.ds(r, STEP), :] = value + decode(ref[pl.ds(i % 2 * rows + r, STEP), :], by)

            chunks(rows, step, None)


def keep(own, came, got):
    rows, cols = own.shape[2:]
    return call(
        keep_body,
        "keep",
        (VMEM((2, RING, rows, cols), F32),),
        [],
        200 * rows * cols,
        80 * rows * cols,
        in_vmem(6),
    )(own, held(came), *[held(g) for g in got])[0]


def middle_body(half, acc, first, second, *refs):
    outs, kept, total = refs[:3], refs[3], refs[4]
    rows, cols = kept.shape
    peaks = []
    for i in range(RING):
        ref = first if i < 2 else second
        by = came_factor(ref.at[2 * rows : 2 * rows + SIDE])[i % 2 : i % 2 + 1]

        def step(r, peak, ref=ref, by=by, i=i):
            value = acc[half, i, pl.ds(r, STEP), :] + decode(ref[pl.ds(i % 2 * rows + r, STEP), :], by)
            if i == 3:
                kept[pl.ds(r, STEP), :] = value
                return peak
            total[i, pl.ds(r, STEP), :] = value
            return jnp.maximum(peak, jnp.abs(value))

        peak = chunks(rows, step, jnp.zeros((STEP, cols), F32))
        if i < 3:
            peaks.append(jnp.max(peak, axis=0, keepdims=True))
    send_blocks(total, outs, peaks, rows, 1)


def middle(acc, first, second, half):
    rows, cols = acc.shape[2:]
    sent = VMEM((rows + SIDE, cols), I16)
    return call(
        functools.partial(middle_body, half),
        "middle",
        (sent, sent, sent, VMEM((rows, cols), F32)),
        [VMEM((3, rows, cols), F32)],
        200 * rows * cols,
        32 * rows * cols,
        in_vmem(3),
    )(acc, held(first), held(second))


def last_body(*refs):
    ins, (grad, squares) = refs[:8], refs[8:]
    rows, cols = ins[0].shape
    square = jnp.zeros((STEP, cols), F32)
    for half in range(2):
        kept, *got = ins[4 * half : 4 * half + 4]
        by = [came_factor(ref.at[rows : rows + SIDE])[0:1] for ref in got]

        def step(r, square, half=half, kept=kept, got=got, by=by):
            value = kept[pl.ds(r, STEP), :]
            for ref, factor in zip(got, by):
                value = value + decode(ref[pl.ds(r, STEP), :], factor)
            grad[0, pl.ds(half * rows + r, STEP), :] = value
            return square + value * value

        square = chunks(rows, step, square)
    folded = square[:, 0:128]
    for at in range(128, cols, 128):
        folded = folded + square[:, at : at + 128]
    squares[...] = jnp.broadcast_to(jnp.sum(folded, axis=0, keepdims=True), squares.shape)


def last(halves, devices):
    rows, cols = halves[0][0].shape
    flat = [a for kept, *got in halves for a in (kept, *[held(g) for g in got])]
    return call(
        last_body,
        "last",
        (VMEM((1, 2 * rows, cols), F32), VMEM((devices, 128), F32)),
        [],
        100 * rows * cols,
        32 * rows * cols,
        in_vmem(8),
    )(*flat)


def reduce_scatter(parts, devices):
    where = jnp.stack([lax.axis_index(a) for a in FSDP]).astype(jnp.int32)
    axis = ("y", "z")

    def hop(value, name, delta):
        return lax.ppermute(value, name, [(i, (i + delta) % RING) for i in range(RING)])

    def four_ways(values):
        return [hop(v, axis[q // 2], 1 if q % 2 == 0 else 3) for q, v in enumerate(values)]

    def swap(value):
        return lax.ppermute(value, "core", [(0, 1), (1, 0)])

    far = tuple((h, 2, low) for h in range(2) for low in (0, 2))
    near = tuple((h, d, low) for h in range(2) for d, low in ((1, 2), (3, 0)))
    join = tuple((h, d, low) for h in range(2) for d, low in ((1, 0), (3, 2)))
    mine = tuple((h, 0, low) for h in range(2) for low in (0, 2))
    (out_far,) = gather(where, parts, ((far, False),))
    came_far = swap(out_far)
    out_near, own_far = gather(where, parts, ((near, False), (far, True)))
    came_near = swap(out_near)
    out_join, own_near = gather(where, parts, ((join, False), (near, True)))
    came_join = swap(out_join)
    out_mine, own_join, own_mine = gather(where, parts, ((mine, False), (join, True), (mine, True)))
    came_mine = swap(out_mine)

    got_far = four_ways(pair(own_far, came_far))
    got_near = four_ways(pair(own_near, came_near))
    got_join = four_ways(pair(own_join, came_join, got_far))
    acc = keep(own_mine, came_mine, got_near)
    halves = []
    for half in range(2):
        *out, kept = middle(acc, got_join[2 * half], got_join[2 * half + 1], half)
        halves.append([kept] + [hop(o, axis[1 - half], d) for o, d in zip(out, ORDER)])
    return last(halves, devices)


def copy_for_each(value, axis):
    copies = jnp.broadcast_to(value, (lax.axis_size(axis), *value.shape))
    return lax.all_to_all(copies, axis, split_axis=0, concat_axis=0, tiled=True)


def of_everyone(value, axis):
    everything = copy_for_each(value, axis)
    return jnp.max(everything, axis=0)


def in_one(arrays, axis):
    flat, at, outs = (jnp.concatenate([a.reshape(-1) for a in arrays]), 0, [])
    total = of_everyone(flat, axis)
    for a in arrays:
        outs.append(total[at : at + a.size].reshape(a.shape))
        at += a.size
    return tuple(outs)


def dequantize(code_values, levels, row_scale, col_scale):
    scale_bound = jnp.minimum(row_scale[:, :, None], col_scale[:, None, :])
    return code_values.astype(jnp.float32) / levels * scale_bound


def moments(
    gradient,
    clip_scale,
    first_codes,
    first_rows,
    first_columns,
    second_codes,
    second_rows,
    second_columns,
):
    first_old = dequantize(first_codes, 7.0, first_rows, first_columns)
    second_old = dequantize(second_codes, 15.0, second_rows, second_columns)
    clipped = clip_scale * gradient
    first_new = beta_first * first_old + (1.0 - beta_first) * clipped
    second_new = beta_second * second_old + (1.0 - beta_second) * clipped * clipped
    direction = first_new / (jnp.sqrt(second_new) + epsilon)
    return (first_new, second_new, direction)


def local(
    grad_parts, first_codes, first_rows, first_columns, second_codes, second_rows, second_columns
):
    layer_count, _, row_count, col_count = grad_parts.shape
    entries = layer_count * lax.axis_size("section") * row_count * col_count
    devices = lax.axis_size(AXES)
    parts = grad_parts.reshape(RING * RING, 2, 2, -1, col_count)
    gradient, squares = reduce_scatter(parts, devices)
    squares = lax.all_to_all(squares, AXES, split_axis=0, concat_axis=0, tiled=True)
    square_sum = jnp.sum(squares)
    clip_limit = clip_rms * math.sqrt(entries)
    clip_scale = clip_limit / jnp.maximum(jnp.sqrt(square_sum), clip_limit)
    first_new, second_new, direction = moments(
        gradient,
        clip_scale,
        first_codes,
        first_rows,
        first_columns,
        second_codes,
        second_rows,
        second_columns,
    )
    first_rowmax = jnp.maximum(jnp.max(jnp.abs(first_new), axis=2), scale_floor)
    first_local = jnp.max(jnp.abs(first_new), axis=1)
    second_rowmax = jnp.max(second_new, axis=2)
    second_local = jnp.max(second_new, axis=1)
    first_colmax, second_colmax = in_one((first_local, second_local), FSDP)
    first_colmax = jnp.maximum(first_colmax, scale_floor)
    first_scaled = first_new / jnp.minimum(first_rowmax[:, :, None], first_colmax[:, None, :])
    second_scaled = second_new / jnp.minimum(second_rowmax[:, :, None], second_colmax[:, None, :])
    return (
        direction,
        first_scaled,
        second_scaled,
        first_rowmax,
        first_colmax,
        second_rowmax,
        second_colmax,
    )


def solution(mesh):
    torus = Mesh(mesh.devices.reshape(mesh.shape["section"], RING, RING, 2), AXES)
    placed = (
        P("section", FSDP, None, None),
        P("section", FSDP, None),
        P("section", FSDP),
        P("section", None),
        P("section", FSDP, None),
        P("section", FSDP),
        P("section", None),
    )
    return jax.shard_map(
        local,
        mesh=torus,
        in_specs=placed,
        out_specs=(
            P("section", FSDP, None),
            P("section", FSDP, None),
            P("section", FSDP, None),
            P("section", FSDP),
            P("section", None),
            P("section", FSDP),
            P("section", None),
        ),
        check_vma=False,
    )
```

```python
import functools
import math

import jax
import jax.numpy as jnp
from jax import lax
from jax.experimental import pallas as pl
from jax.experimental.pallas import tpu as pltpu
from jax.sharding import Mesh
from jax.sharding import PartitionSpec as P


AXES = ("section", "y", "z", "core")
FSDP = ("y", "z", "core")

beta_first = 0.9
beta_second = 0.999
clip_rms = 3.0
epsilon = 1e-08
scale_floor = 0.001

RING = 4
ORDER = (1, 3, 2, 0)
TOP = 32767.0
LEAST = 1e-18
SIDE = 8
STEP = 64
VMEM_LIMIT = 20 * 1024 * 1024
F32, I16 = jnp.float32, jnp.int16
VMEM = pltpu.VMEM


def scale_code(peak):
    return jnp.ceil(jnp.log2(jnp.maximum(peak, LEAST)) * 256.0)


def send_factor(code):
    return jnp.exp2(code * (-1.0 / 256.0)) * TOP**4


def encode(values, factor):
    root = lax.rsqrt(lax.rsqrt(jnp.abs(values) * factor))
    root = jnp.where(values < 0.0, -root, root)
    return jnp.round(root).astype(jnp.int32).astype(I16)


def came_factor(side):
    code = side[...].astype(jnp.int32).astype(F32)
    return jnp.exp2(code * (1.0 / 256.0)) * TOP**-4


def decode(codes, factor):
    root = codes.astype(jnp.int32).astype(F32)
    square = root * jnp.abs(root)
    return (square * jnp.abs(square)) * factor


def side_rows(codes):
    line = lax.broadcasted_iota(jnp.int32, (SIDE, codes[0].shape[1]), 0)
    rows = codes[-1]
    for at, code in enumerate(codes[:-1]):
        rows = jnp.where(line == at, code, rows)
    return jnp.broadcast_to(rows, line.shape).astype(jnp.int32).astype(I16)


def call(body, outs, scratch, flops, bytes_accessed, in_specs):
    return pl.pallas_call(
        body,
        out_shape=outs,
        in_specs=in_specs,
        out_specs=tuple(pl.BlockSpec(memory_space=VMEM) for _ in outs),
        scratch_shapes=scratch,
        compiler_params=pltpu.CompilerParams(vmem_limit_bytes=VMEM_LIMIT),
        cost_estimate=pl.CostEstimate(flops=flops, bytes_accessed=bytes_accessed, transcendentals=0),
    )


def in_vmem(n):
    return [pl.BlockSpec(memory_space=VMEM)] * n


def held(value):
    return pltpu.with_memory_space_constraint(value, VMEM)


def gather_copies(wanted, where, parts, outs, sem):
    copies = []
    for (jobs, mine), out in zip(wanted, outs):
        core = where[2] if mine else 1 - where[2]
        for q, (half, delta, low) in enumerate(jobs):
            for i in range(2):
                j = lax.rem(where[1 - half] + ORDER[low + i], RING)
                far = lax.rem(where[half] + delta, RING)
                at = far * RING + j if half == 0 else j * RING + far
                copies.append(
                    pltpu.make_async_copy(
                        parts.at[at, core, half], out.at[q, i], sem.at[len(copies)]
                    )
                )
    return copies


def gather_body(wanted, where, parts, *refs):
    copies = gather_copies(wanted, where, parts, refs[:-1], refs[-1])
    for copy in copies:
        copy.start()
    for copy in copies:
        copy.wait()


def gather_specs():
    return [pl.BlockSpec(memory_space=pltpu.SMEM), pl.BlockSpec(memory_space=pltpu.HBM)]


def gather_outs(parts, wanted):
    rows, cols = parts.shape[3:]
    return (
        tuple(VMEM((4, 2, rows, cols), parts.dtype) for _ in wanted),
        pltpu.SemaphoreType.DMA((8 * len(wanted),)),
        32 * len(wanted) * rows * cols,
    )


def gather(where, parts, wanted):
    outs, sem, moved = gather_outs(parts, wanted)
    body = functools.partial(gather_body, wanted)
    return call(body, outs, [sem], moved // 4, moved, gather_specs())(where, parts)


def chunks(rows, step, carry):
    return lax.fori_loop(0, rows // STEP, lambda n, c: step(pl.multiple_of(n * STEP, STEP), c), carry)


def fold(values, join):
    folded = values[0:8]
    for at in range(8, values.shape[0], 8):
        folded = join(folded, values[at : at + 8])
    return folded


def send_blocks(total, outs, peaks, rows, each):
    code = scale_code(jnp.concatenate(peaks, axis=0))
    factor = send_factor(code)
    for q, out in enumerate(outs):
        for i in range(each):
            line = q * each + i
            by = factor[line : line + 1]

            def step(r, _, line=line, by=by, out=out, i=i):
                out[pl.ds(i * rows + r, STEP), :] = encode(total[line, pl.ds(r, STEP), :], by)

            chunks(rows, step, None)
        out[each * rows : each * rows + SIDE, :] = side_rows(
            [code[q * each + i : q * each + i + 1] for i in range(each)]
        )


def pair_body(relays, wanted, *refs):
    own, came = refs[:2]
    relayed, refs = refs[2 : 2 + relays], refs[2 + relays :]
    copies = []
    if wanted:
        (where, parts), refs = refs[:2], refs[2:]
        copies = gather_copies(wanted, where, parts, refs[4 : 4 + len(wanted)], refs[-1])
    for copy in copies:
        copy.start()
    outs, total = refs[:4], refs[4 + len(wanted)]
    rows, cols = own.shape[2:]
    peaks = []
    for q in range(4):
        by = came_factor(relayed[q].at[2 * rows : 2 * rows + SIDE]) if relayed else None
        for i in range(2):

            def step(r, peak, q=q, i=i, by=by):
                value = own[q, i, pl.ds(r, STEP), :].astype(F32) + came[q, i, pl.ds(r, STEP), :].astype(F32)
                if relayed:
                    value = value + decode(relayed[q][pl.ds(i * rows + r, STEP), :], by[i : i + 1])
                total[2 * q + i, pl.ds(r, STEP), :] = value
                return jnp.maximum(peak, fold(jnp.abs(value), jnp.maximum))

            peak = chunks(rows, step, jnp.zeros((8, cols), F32))
            peaks.append(jnp.max(peak, axis=0, keepdims=True))
    send_blocks(total, outs, peaks, rows, 2)
    for copy in copies:
        copy.wait()


def pair(own, came, relayed=(), where=None, parts=None, wanted=()):
    rows, cols = own.shape[2:]
    outs, scratch = (VMEM((2 * rows + SIDE, cols), I16),) * 4, [VMEM((8, rows, cols), F32)]
    specs, args = in_vmem(2 + len(relayed)), [own, held(came), *[held(r) for r in relayed]]
    if wanted:
        more, sem, _ = gather_outs(parts, wanted)
        outs, scratch = outs + more, scratch + [sem]
        specs, args = specs + gather_specs(), args + [where, parts]
    got = call(
        functools.partial(pair_body, len(relayed), wanted), outs, scratch, 400 * rows * cols, 48 * rows * cols, specs
    )(*args)
    return got[:4], got[4:]


def column_of(row):
    n = row.shape[1]
    return jnp.transpose(jnp.broadcast_to(row, (128, n)))[:, 0:1]


def row_of(column):
    n = column.shape[0]
    return jnp.transpose(jnp.broadcast_to(column, (n, 128)))[0:1, :]


def keep_body(own, came, *refs):
    got, (old, total, first_old, second_old) = refs[:4], (refs[4:10], *refs[10:])
    rows = own.shape[2]
    for half in range(2):
        for i in range(RING):
            ref = got[2 * half + (1 if i < 2 else 0)]
            by = came_factor(ref.at[2 * rows : 2 * rows + SIDE])[i % 2 : i % 2 + 1]

            def step(r, _, ref=ref, by=by, half=half, i=i):
                q = 2 * half + i // 2
                value = own[q, i % 2, pl.ds(r, STEP), :].astype(F32) + came[q, i % 2, pl.ds(r, STEP), :].astype(F32)
                total[half, i, pl.ds(r, STEP), :] = value + decode(ref[pl.ds(i % 2 * rows + r, STEP), :], by)

            chunks(rows, step, None)
    for (codes, row, column), levels, beta, out in (
        (old[:3], 7.0, beta_first, first_old),
        (old[3:], 15.0, beta_second, second_old),
    ):
        tall, wide = column_of(row[...]), column[...]
        for r in range(0, out.shape[0], STEP):
            bound = jnp.minimum(tall[r : r + STEP], wide)
            out[r : r + STEP, :] = codes[0, r : r + STEP, :].astype(F32) * (beta / levels) * bound


def keep(own, came, got, old):
    rows, cols = own.shape[2:]
    each = VMEM((2 * rows, cols), F32)
    return call(
        keep_body, (VMEM((2, RING, rows, cols), F32), each, each), [], 300 * rows * cols, 100 * rows * cols, in_vmem(12)
    )(own, held(came), *[held(g) for g in got], *old)


def middle_body(half, acc, first, second, *refs):
    outs, kept, total = refs[:3], refs[3], refs[4]
    rows, cols = kept.shape
    peaks = []
    for i in range(RING):
        ref = first if i < 2 else second
        by = came_factor(ref.at[2 * rows : 2 * rows + SIDE])[i % 2 : i % 2 + 1]

        def step(r, peak, ref=ref, by=by, i=i):
            value = acc[half, i, pl.ds(r, STEP), :] + decode(ref[pl.ds(i % 2 * rows + r, STEP), :], by)
            if i == 3:
                kept[pl.ds(r, STEP), :] = value
                return peak
            total[i, pl.ds(r, STEP), :] = value
            return jnp.maximum(peak, fold(jnp.abs(value), jnp.maximum))

        peak = chunks(rows, step, jnp.zeros((8, cols), F32))
        if i < 3:
            peaks.append(jnp.max(peak, axis=0, keepdims=True))
    send_blocks(total, outs, peaks, rows, 1)


def middle(acc, first, second, half):
    rows, cols = acc.shape[2:]
    sent = VMEM((rows + SIDE, cols), I16)
    return call(
        functools.partial(middle_body, half),
        (sent, sent, sent, VMEM((rows, cols), F32)),
        [VMEM((3, rows, cols), F32)],
        200 * rows * cols,
        32 * rows * cols,
        in_vmem(3),
    )(acc, held(first), held(second))


def last_body(*refs):
    ins, (grad, squares) = refs[:8], refs[8:]
    rows, cols = ins[0].shape
    square = jnp.zeros((8, cols), F32)
    for half in range(2):
        kept, *got = ins[4 * half : 4 * half + 4]
        by = [came_factor(ref.at[rows : rows + SIDE])[0:1] for ref in got]

        def step(r, square, half=half, kept=kept, got=got, by=by):
            value = kept[pl.ds(r, STEP), :]
            for ref, factor in zip(got, by):
                value = value + decode(ref[pl.ds(r, STEP), :], factor)
            grad[pl.ds(half * rows + r, STEP), :] = value
            return square + fold(value * value, jnp.add)

        square = chunks(rows, step, square)
    folded = square[:, 0:128]
    for at in range(128, cols, 128):
        folded = folded + square[:, at : at + 128]
    squares[...] = jnp.broadcast_to(jnp.sum(folded, axis=0, keepdims=True), squares.shape)


def last(halves, devices):
    rows, cols = halves[0][0].shape
    flat = [a for kept, *got in halves for a in (kept, *[held(g) for g in got])]
    return call(
        last_body,
        (VMEM((2 * rows, cols), F32), VMEM((devices, 128), F32)),
        [],
        100 * rows * cols,
        32 * rows * cols,
        in_vmem(8),
    )(*flat)


def reduce_scatter(parts, old, devices):
    where = jnp.stack([lax.axis_index(a) for a in FSDP]).astype(jnp.int32)
    parts = pltpu.with_memory_space_constraint(parts, pltpu.HBM)
    axis = ("y", "z")

    def hop(value, name, delta):
        return lax.ppermute(value, name, [(i, (i + delta) % RING) for i in range(RING)])

    def four_ways(values):
        return [hop(v, axis[q // 2], 1 if q % 2 == 0 else 3) for q, v in enumerate(values)]

    def swap(value):
        return lax.ppermute(value, "core", [(0, 1), (1, 0)])

    far = tuple((h, 2, low) for h in range(2) for low in (0, 2))
    near = tuple((h, d, low) for h in range(2) for d, low in ((1, 2), (3, 0)))
    join = tuple((h, d, low) for h in range(2) for d, low in ((1, 0), (3, 2)))
    mine = tuple((h, 0, low) for h in range(2) for low in (0, 2))
    (out_far,) = gather(where, parts, ((far, False),))
    came_far = swap(out_far)
    out_near, own_far = gather(where, parts, ((near, False), (far, True)))
    came_near = swap(out_near)
    sent, (out_join, own_near) = pair(
        own_far, came_far, (), where, parts, ((join, False), (near, True))
    )
    got_far = four_ways(sent)
    came_join = swap(out_join)
    sent, (out_mine, own_join, own_mine) = pair(
        own_near, came_near, (), where, parts, ((mine, False), (join, True), (mine, True))
    )
    got_near = four_ways(sent)
    came_mine = swap(out_mine)
    sent, _ = pair(own_join, came_join, got_far)
    got_join = four_ways(sent)
    acc, first_old, second_old = keep(own_mine, came_mine, got_near, old)
    halves = []
    for half in range(2):
        *out, kept = middle(acc, got_join[2 * half], got_join[2 * half + 1], half)
        got = {d: hop(out[k], axis[1 - half], d) for k, d in ((2, 2), (0, 1), (1, 3))}
        halves.append([kept, got[1], got[3], got[2]])
    return *last(halves, devices), first_old, second_old


def clip_body(limit, squares, grad, first_old, second_old, first_new, second_new, peaks):
    rows, cols = grad.shape
    total = jnp.sum(jnp.sum(squares[...], axis=0, keepdims=True), axis=1, keepdims=True)
    scale = limit / jnp.maximum(jnp.sqrt(total), limit)

    def step(r, peak):
        clipped = grad[pl.ds(r, STEP), :] * scale
        first = first_old[pl.ds(r, STEP), :] + (1.0 - beta_first) * clipped
        second = second_old[pl.ds(r, STEP), :] + (1.0 - beta_second) * clipped * clipped
        first_new[pl.ds(r, STEP), :] = first
        second_new[pl.ds(r, STEP), :] = second
        return (
            jnp.maximum(peak[0], fold(jnp.abs(first), jnp.maximum)),
            jnp.maximum(peak[1], fold(second, jnp.maximum)),
        )

    zero = jnp.zeros((8, cols), F32)
    found = chunks(rows, step, (zero, zero))
    lines = []
    for peak in found:
        peak = jnp.max(peak, axis=0, keepdims=True)
        lines += [peak[:, at : at + 128] for at in range(0, cols, 128)]
    lines = jnp.concatenate(lines, axis=0)
    for at in range(peaks.shape[0]):
        peaks[at] = lines


def clip(squares, grad, first_old, second_old, limit, group):
    rows, cols = grad.shape
    each = VMEM((rows, cols), F32)
    return call(
        functools.partial(clip_body, limit),
        (each, each, VMEM((group, 2 * cols // 128, 128), F32)),
        [],
        12 * rows * cols,
        20 * rows * cols,
        in_vmem(4),
    )(held(squares), grad, first_old, second_old)


def rows_body(first_new, second_new, direction, first_rowmax, second_rowmax, by_first, by_second):
    first, second = first_new[...], second_new[...]
    direction[0] = first / (jnp.sqrt(second) + epsilon)
    for values, least, peak, by in (
        (jnp.abs(first), scale_floor, first_rowmax, by_first),
        (second, 0.0, second_rowmax, by_second),
    ):
        tall = jnp.maximum(jnp.max(values, axis=1, keepdims=True), least)
        by[...] = jnp.broadcast_to(1.0 / tall, by.shape)
        peak[...] = row_of(tall)


def row_outputs(first_new, second_new):
    rows, cols = first_new.shape
    step = min(rows, 128)
    whole = pl.BlockSpec((step, cols), lambda r: (r, 0))
    side, line = pl.BlockSpec((step, 128), lambda r: (r, 0)), pl.BlockSpec((1, step), lambda r: (0, r))
    return pl.pallas_call(
        rows_body,
        grid=(rows // step,),
        out_shape=(
            jax.ShapeDtypeStruct((1, rows, cols), F32),
            jax.ShapeDtypeStruct((1, rows), F32),
            jax.ShapeDtypeStruct((1, rows), F32),
            VMEM((rows, 128), F32),
            VMEM((rows, 128), F32),
        ),
        in_specs=[whole, whole],
        out_specs=(pl.BlockSpec((1, step, cols), lambda r: (0, r, 0)), line, line, side, side),
        compiler_params=pltpu.CompilerParams(vmem_limit_bytes=VMEM_LIMIT),
        cost_estimate=pl.CostEstimate(flops=40 * rows * cols, bytes_accessed=12 * rows * cols, transcendentals=0),
        name="row_outputs",
    )(first_new, second_new)


def scaled_body(peaks, first_new, second_new, by_first, by_second, *refs):
    first_scaled, second_scaled, first_colmax, second_colmax, inverse = refs
    half = peaks.shape[1] // 2

    @pl.when(pl.program_id(0) == 0)
    def _():
        found = jnp.max(peaks[...], axis=0)
        for k, (out, least) in enumerate(((first_colmax, scale_floor), (second_colmax, 0.0))):
            wide = [found[k * half + at : k * half + at + 1] for at in range(half)]
            wide = jnp.maximum(jnp.concatenate(wide, axis=1), least)
            out[...] = wide
            inverse[k : k + 1, :] = 1.0 / wide

    for k, (values, by, out) in enumerate(
        ((first_new, by_first, first_scaled), (second_new, by_second, second_scaled))
    ):
        out[0] = values[...] * jnp.maximum(by[:, 0:1], inverse[k : k + 1, :])


def scaled_outputs(peaks, first_new, second_new, by_first, by_second):
    rows, cols = first_new.shape
    step = min(rows, 64)
    whole, side = pl.BlockSpec((step, cols), lambda r: (r, 0)), pl.BlockSpec((step, 128), lambda r: (r, 0))
    out, line = pl.BlockSpec((1, step, cols), lambda r: (0, r, 0)), pl.BlockSpec((1, cols), lambda r: (0, 0))
    big, wide = jax.ShapeDtypeStruct((1, rows, cols), F32), jax.ShapeDtypeStruct((1, cols), F32)
    return pl.pallas_call(
        scaled_body,
        grid=(rows // step,),
        out_shape=(big, big, wide, wide),
        in_specs=[pl.BlockSpec(memory_space=VMEM), whole, whole, side, side],
        out_specs=(out, out, line, line),
        scratch_shapes=[VMEM((8, cols), F32)],
        compiler_params=pltpu.CompilerParams(vmem_limit_bytes=VMEM_LIMIT),
        cost_estimate=pl.CostEstimate(flops=8 * rows * cols, bytes_accessed=16 * rows * cols, transcendentals=0),
        name="scaled_outputs",
    )(held(peaks), first_new, second_new, by_first, by_second)


def exchange(value, axes):
    return lax.all_to_all(value, axes, split_axis=0, concat_axis=0, tiled=True)


def local(
    grad_parts, first_codes, first_rows, first_columns, second_codes, second_rows, second_columns
):
    layer_count, _, row_count, col_count = grad_parts.shape
    entries = layer_count * lax.axis_size("section") * row_count * col_count
    devices, group = lax.axis_size(AXES), lax.axis_size(FSDP)
    parts = grad_parts.reshape(RING * RING, 2, 2, -1, col_count)
    old = (first_codes, first_rows, first_columns, second_codes, second_rows, second_columns)
    gradient, squares, first_old, second_old = reduce_scatter(parts, old, devices)
    squares = exchange(squares, AXES)
    clip_limit = clip_rms * math.sqrt(entries)
    first_new, second_new, peaks = clip(squares, gradient, first_old, second_old, clip_limit, group)
    peaks = exchange(peaks, FSDP)
    direction, first_rowmax, second_rowmax, by_first, by_second = row_outputs(first_new, second_new)
    first_scaled, second_scaled, first_colmax, second_colmax = scaled_outputs(
        peaks, first_new, second_new, by_first, by_second
    )
    return (
        direction,
        first_scaled,
        second_scaled,
        first_rowmax,
        first_colmax,
        second_rowmax,
        second_colmax,
    )


def solution(mesh):
    torus = Mesh(mesh.devices.reshape(mesh.shape["section"], RING, RING, 2), AXES)
    placed = (
        P("section", FSDP, None, None),
        P("section", FSDP, None),
        P("section", FSDP),
        P("section", None),
        P("section", FSDP, None),
        P("section", FSDP),
        P("section", None),
    )
    return jax.shard_map(
        local,
        mesh=torus,
        in_specs=placed,
        out_specs=(
            P("section", FSDP, None),
            P("section", FSDP, None),
            P("section", FSDP, None),
            P("section", FSDP),
            P("section", None),
            P("section", FSDP),
            P("section", None),
        ),
        check_vma=False,
    )
```

```python
import functools
import math

import jax
import jax.numpy as jnp
from jax import lax
from jax.experimental import pallas as pl
from jax.experimental.pallas import tpu as pltpu
from jax.sharding import Mesh
from jax.sharding import PartitionSpec as P


AXES = ("section", "y", "z", "core")
FSDP = ("y", "z", "core")

beta_first = 0.9
beta_second = 0.999
clip_rms = 3.0
epsilon = 1e-08
scale_floor = 0.001

RING = 4
ORDER = (1, 3, 2, 0)
TOP = 32767.0
LEAST = 1e-18
SIDE = 8
STEP = 64
VMEM_LIMIT = 20 * 1024 * 1024
F32, I16 = jnp.float32, jnp.int16
VMEM = pltpu.VMEM


def scale_code(peak):
    return jnp.ceil(jnp.log2(jnp.maximum(peak, LEAST)) * 256.0)


def send_factor(code):
    return jnp.exp2(code * (-1.0 / 256.0)) * TOP**4


def encode(values, factor):
    root = lax.rsqrt(lax.rsqrt(jnp.abs(values) * factor))
    root = jnp.where(values < 0.0, -root, root)
    return jnp.round(root).astype(jnp.int32).astype(I16)


def came_factor(side):
    code = side[...].astype(jnp.int32).astype(F32)
    return jnp.exp2(code * (1.0 / 256.0)) * TOP**-4


def decode(codes, factor):
    root = codes.astype(jnp.int32).astype(F32)
    square = root * jnp.abs(root)
    return (square * jnp.abs(square)) * factor


def side_rows(codes):
    line = lax.broadcasted_iota(jnp.int32, (SIDE, codes[0].shape[1]), 0)
    rows = codes[-1]
    for at, code in enumerate(codes[:-1]):
        rows = jnp.where(line == at, code, rows)
    return jnp.broadcast_to(rows, line.shape).astype(jnp.int32).astype(I16)


def call(body, outs, scratch, flops, bytes_accessed, in_specs):
    return pl.pallas_call(
        body,
        out_shape=outs,
        in_specs=in_specs,
        out_specs=tuple(pl.BlockSpec(memory_space=VMEM) for _ in outs),
        scratch_shapes=scratch,
        compiler_params=pltpu.CompilerParams(vmem_limit_bytes=VMEM_LIMIT),
        cost_estimate=pl.CostEstimate(flops=flops, bytes_accessed=bytes_accessed, transcendentals=0),
    )


def in_vmem(n):
    return [pl.BlockSpec(memory_space=VMEM)] * n


def held(value):
    return pltpu.with_memory_space_constraint(value, VMEM)


def gather_copies(wanted, where, parts, outs, sem):
    copies = []
    for (jobs, mine), out in zip(wanted, outs):
        core = where[2] if mine else 1 - where[2]
        for q, (half, delta, low) in enumerate(jobs):
            for i in range(2):
                j = lax.rem(where[1 - half] + ORDER[low + i], RING)
                far = lax.rem(where[half] + delta, RING)
                at = far * RING + j if half == 0 else j * RING + far
                copies.append(
                    pltpu.make_async_copy(
                        parts.at[at, core, half], out.at[q, i], sem.at[len(copies)]
                    )
                )
    return copies


def gather_body(wanted, where, parts, *refs):
    copies = gather_copies(wanted, where, parts, refs[:-1], refs[-1])
    for copy in copies:
        copy.start()
    for copy in copies:
        copy.wait()


def gather_specs():
    return [pl.BlockSpec(memory_space=pltpu.SMEM), pl.BlockSpec(memory_space=pltpu.HBM)]


def gather_outs(parts, wanted):
    rows, cols = parts.shape[3:]
    return (
        tuple(VMEM((4, 2, rows, cols), parts.dtype) for _ in wanted),
        pltpu.SemaphoreType.DMA((8 * len(wanted),)),
        32 * len(wanted) * rows * cols,
    )


def gather(where, parts, wanted):
    outs, sem, moved = gather_outs(parts, wanted)
    body = functools.partial(gather_body, wanted)
    return call(body, outs, [sem], moved // 4, moved, gather_specs())(where, parts)


def chunks(rows, step, carry):
    return lax.fori_loop(0, rows // STEP, lambda n, c: step(pl.multiple_of(n * STEP, STEP), c), carry)


def fold(values, join):
    folded = values[0:8]
    for at in range(8, values.shape[0], 8):
        folded = join(folded, values[at : at + 8])
    return folded


def send_blocks(total, outs, peaks, rows, each):
    code = scale_code(jnp.concatenate(peaks, axis=0))
    factor = send_factor(code)
    for q, out in enumerate(outs):
        for i in range(each):
            line = q * each + i
            by = factor[line : line + 1]

            def step(r, _, line=line, by=by, out=out, i=i):
                out[pl.ds(i * rows + r, STEP), :] = encode(total[line, pl.ds(r, STEP), :], by)

            chunks(rows, step, None)
        out[each * rows : each * rows + SIDE, :] = side_rows(
            [code[q * each + i : q * each + i + 1] for i in range(each)]
        )


def pair_body(relays, wanted, *refs):
    own, came = refs[:2]
    relayed, refs = refs[2 : 2 + relays], refs[2 + relays :]
    copies = []
    if wanted:
        (where, parts), refs = refs[:2], refs[2:]
        copies = gather_copies(wanted, where, parts, refs[4 : 4 + len(wanted)], refs[-1])
    for copy in copies:
        copy.start()
    outs, total = refs[:4], refs[4 + len(wanted)]
    rows, cols = own.shape[2:]
    peaks = []
    for q in range(4):
        by = came_factor(relayed[q].at[2 * rows : 2 * rows + SIDE]) if relayed else None
        for i in range(2):

            def step(r, peak, q=q, i=i, by=by):
                value = own[q, i, pl.ds(r, STEP), :].astype(F32) + came[q, i, pl.ds(r, STEP), :].astype(F32)
                if relayed:
                    value = value + decode(relayed[q][pl.ds(i * rows + r, STEP), :], by[i : i + 1])
                total[2 * q + i, pl.ds(r, STEP), :] = value
                return jnp.maximum(peak, fold(jnp.abs(value), jnp.maximum))

            peak = chunks(rows, step, jnp.zeros((8, cols), F32))
            peaks.append(jnp.max(peak, axis=0, keepdims=True))
    send_blocks(total, outs, peaks, rows, 2)
    for copy in copies:
        copy.wait()


def pair(own, came, relayed=(), where=None, parts=None, wanted=()):
    rows, cols = own.shape[2:]
    outs, scratch = (VMEM((2 * rows + SIDE, cols), I16),) * 4, [VMEM((8, rows, cols), F32)]
    specs, args = in_vmem(2 + len(relayed)), [own, held(came), *[held(r) for r in relayed]]
    if wanted:
        more, sem, _ = gather_outs(parts, wanted)
        outs, scratch = outs + more, scratch + [sem]
        specs, args = specs + gather_specs(), args + [where, parts]
    got = call(
        functools.partial(pair_body, len(relayed), wanted), outs, scratch, 400 * rows * cols, 48 * rows * cols, specs
    )(*args)
    return got[:4], got[4:]


def column_of(row):
    n = row.shape[1]
    return jnp.transpose(jnp.broadcast_to(row, (128, n)))[:, 0:1]


def row_of(column):
    n = column.shape[0]
    return jnp.transpose(jnp.broadcast_to(column, (n, 128)))[0:1, :]


def keep_body(own, came, *refs):
    got, total = refs[:4], refs[4]
    rows = own.shape[2]
    for half in range(2):
        for i in range(RING):
            ref = got[2 * half + (1 if i < 2 else 0)]
            by = came_factor(ref.at[2 * rows : 2 * rows + SIDE])[i % 2 : i % 2 + 1]

            def step(r, _, ref=ref, by=by, half=half, i=i):
                q = 2 * half + i // 2
                value = own[q, i % 2, pl.ds(r, STEP), :].astype(F32) + came[q, i % 2, pl.ds(r, STEP), :].astype(F32)
                total[half, i, pl.ds(r, STEP), :] = value + decode(ref[pl.ds(i % 2 * rows + r, STEP), :], by)

            chunks(rows, step, None)


def keep(own, came, got):
    rows, cols = own.shape[2:]
    return call(
        keep_body, (VMEM((2, RING, rows, cols), F32),), [], 200 * rows * cols, 80 * rows * cols, in_vmem(6)
    )(own, held(came), *[held(g) for g in got])[0]


def old_body(*refs):
    for (codes, row, column, out), levels, beta in (
        ((*refs[:3], refs[6]), 7.0, beta_first),
        ((*refs[3:6], refs[7]), 15.0, beta_second),
    ):
        tall, wide = column_of(row[...]), column[...]
        for r in range(0, out.shape[0], STEP):
            bound = jnp.minimum(tall[r : r + STEP], wide)
            out[r : r + STEP, :] = codes[0, r : r + STEP, :].astype(F32) * (beta / levels) * bound


def old_moments(old):
    _, rows, cols = old[0].shape
    each = VMEM((rows, cols), F32)
    return call(old_body, (each, each), [], 10 * rows * cols, 16 * rows * cols, in_vmem(6))(*old)


def middle_body(half, acc, first, second, *refs):
    outs, kept, total = refs[:3], refs[3], refs[4]
    rows, cols = kept.shape
    peaks = []
    for i in range(RING):
        ref = first if i < 2 else second
        by = came_factor(ref.at[2 * rows : 2 * rows + SIDE])[i % 2 : i % 2 + 1]

        def step(r, peak, ref=ref, by=by, i=i):
            value = acc[half, i, pl.ds(r, STEP), :] + decode(ref[pl.ds(i % 2 * rows + r, STEP), :], by)
            if i == 3:
                kept[pl.ds(r, STEP), :] = value
                return peak
            total[i, pl.ds(r, STEP), :] = value
            return jnp.maximum(peak, fold(jnp.abs(value), jnp.maximum))

        peak = chunks(rows, step, jnp.zeros((8, cols), F32))
        if i < 3:
            peaks.append(jnp.max(peak, axis=0, keepdims=True))
    send_blocks(total, outs, peaks, rows, 1)


def middle(acc, first, second, half):
    rows, cols = acc.shape[2:]
    sent = VMEM((rows + SIDE, cols), I16)
    return call(
        functools.partial(middle_body, half),
        (sent, sent, sent, VMEM((rows, cols), F32)),
        [VMEM((3, rows, cols), F32)],
        200 * rows * cols,
        32 * rows * cols,
        in_vmem(3),
    )(acc, held(first), held(second))


def last_body(*refs):
    ins, (grad, squares) = refs[:8], refs[8:]
    rows, cols = ins[0].shape
    square = jnp.zeros((8, cols), F32)
    for half in range(2):
        kept, *got = ins[4 * half : 4 * half + 4]
        by = [came_factor(ref.at[rows : rows + SIDE])[0:1] for ref in got]

        def step(r, square, half=half, kept=kept, got=got, by=by):
            value = kept[pl.ds(r, STEP), :]
            for ref, factor in zip(got, by):
                value = value + decode(ref[pl.ds(r, STEP), :], factor)
            grad[pl.ds(half * rows + r, STEP), :] = value
            return square + fold(value * value, jnp.add)

        square = chunks(rows, step, square)
    folded = square[:, 0:128]
    for at in range(128, cols, 128):
        folded = folded + square[:, at : at + 128]
    squares[...] = jnp.broadcast_to(jnp.sum(folded, axis=0, keepdims=True), squares.shape)


def last(halves, devices):
    rows, cols = halves[0][0].shape
    flat = [a for kept, *got in halves for a in (kept, *[held(g) for g in got])]
    return call(
        last_body,
        (VMEM((2 * rows, cols), F32), VMEM((devices, 128), F32)),
        [],
        100 * rows * cols,
        32 * rows * cols,
        in_vmem(8),
    )(*flat)


def reduce_scatter(parts, devices):
    where = jnp.stack([lax.axis_index(a) for a in FSDP]).astype(jnp.int32)
    parts = pltpu.with_memory_space_constraint(parts, pltpu.HBM)
    axis = ("y", "z")

    def hop(value, name, delta):
        return lax.ppermute(value, name, [(i, (i + delta) % RING) for i in range(RING)])

    def four_ways(values):
        return [hop(v, axis[q // 2], 1 if q % 2 == 0 else 3) for q, v in enumerate(values)]

    def swap(value):
        return lax.ppermute(value, "core", [(0, 1), (1, 0)])

    far = tuple((h, 2, low) for h in range(2) for low in (0, 2))
    near = tuple((h, d, low) for h in range(2) for d, low in ((1, 2), (3, 0)))
    join = tuple((h, d, low) for h in range(2) for d, low in ((1, 0), (3, 2)))
    mine = tuple((h, 0, low) for h in range(2) for low in (0, 2))
    (out_far,) = gather(where, parts, ((far, False),))
    came_far = swap(out_far)
    out_near, own_far = gather(where, parts, ((near, False), (far, True)))
    came_near = swap(out_near)
    sent, (out_join, own_near) = pair(
        own_far, came_far, (), where, parts, ((join, False), (near, True))
    )
    got_far = four_ways(sent)
    came_join = swap(out_join)
    sent, (out_mine, own_join, own_mine) = pair(
        own_near, came_near, (), where, parts, ((mine, False), (join, True), (mine, True))
    )
    got_near = four_ways(sent)
    came_mine = swap(out_mine)
    sent, _ = pair(own_join, came_join, got_far)
    got_join = four_ways(sent)
    acc = keep(own_mine, came_mine, got_near)
    halves = []
    for half in range(2):
        *out, kept = middle(acc, got_join[2 * half], got_join[2 * half + 1], half)
        got = [hop(out[2], axis[1 - half], 2)]
        got += [hop(out[0], axis[1 - half], 1), hop(out[1], axis[1 - half], 3)]
        halves.append([kept] + got)
    return last(halves, devices)


def clip_body(limit, squares, grad, first_old, second_old, first_new, second_new, peaks):
    rows, cols = grad.shape
    total = jnp.sum(jnp.sum(squares[...], axis=0, keepdims=True), axis=1, keepdims=True)
    scale = limit / jnp.maximum(jnp.sqrt(total), limit)

    def step(r, peak):
        clipped = grad[pl.ds(r, STEP), :] * scale
        first = first_old[pl.ds(r, STEP), :] + (1.0 - beta_first) * clipped
        second = second_old[pl.ds(r, STEP), :] + (1.0 - beta_second) * clipped * clipped
        first_new[pl.ds(r, STEP), :] = first
        second_new[pl.ds(r, STEP), :] = second
        return (
            jnp.maximum(peak[0], fold(jnp.abs(first), jnp.maximum)),
            jnp.maximum(peak[1], fold(second, jnp.maximum)),
        )

    zero = jnp.zeros((8, cols), F32)
    found = chunks(rows, step, (zero, zero))
    lines = []
    for peak in found:
        peak = jnp.max(peak, axis=0, keepdims=True)
        lines += [peak[:, at : at + 128] for at in range(0, cols, 128)]
    lines = jnp.concatenate(lines, axis=0)
    for at in range(peaks.shape[0]):
        peaks[at] = lines


def clip(squares, grad, first_old, second_old, limit, group):
    rows, cols = grad.shape
    each = VMEM((rows, cols), F32)
    return call(
        functools.partial(clip_body, limit),
        (each, each, VMEM((group, 2 * cols // 128, 128), F32)),
        [],
        12 * rows * cols,
        20 * rows * cols,
        in_vmem(4),
    )(held(squares), grad, first_old, second_old)


def rows_body(first_new, second_new, direction, first_rowmax, second_rowmax, by_first, by_second):
    first, second = first_new[...], second_new[...]
    direction[0] = first / (jnp.sqrt(second) + epsilon)
    for values, least, peak, by in (
        (jnp.abs(first), scale_floor, first_rowmax, by_first),
        (second, 0.0, second_rowmax, by_second),
    ):
        tall = jnp.maximum(jnp.max(values, axis=1, keepdims=True), least)
        by[...] = jnp.broadcast_to(1.0 / tall, by.shape)
        peak[...] = row_of(tall)


def row_outputs(first_new, second_new):
    rows, cols = first_new.shape
    step = min(rows, 128)
    whole = pl.BlockSpec((step, cols), lambda r: (r, 0))
    side, line = pl.BlockSpec((step, 128), lambda r: (r, 0)), pl.BlockSpec((1, step), lambda r: (0, r))
    return pl.pallas_call(
        rows_body,
        grid=(rows // step,),
        out_shape=(
            jax.ShapeDtypeStruct((1, rows, cols), F32),
            jax.ShapeDtypeStruct((1, rows), F32),
            jax.ShapeDtypeStruct((1, rows), F32),
            VMEM((rows, 128), F32),
            VMEM((rows, 128), F32),
        ),
        in_specs=[whole, whole],
        out_specs=(pl.BlockSpec((1, step, cols), lambda r: (0, r, 0)), line, line, side, side),
        compiler_params=pltpu.CompilerParams(vmem_limit_bytes=VMEM_LIMIT),
        cost_estimate=pl.CostEstimate(flops=40 * rows * cols, bytes_accessed=12 * rows * cols, transcendentals=0),
        name="row_outputs",
    )(first_new, second_new)


def scaled_body(peaks, first_new, second_new, by_first, by_second, *refs):
    first_scaled, second_scaled, first_colmax, second_colmax, inverse = refs
    half = peaks.shape[1] // 2

    @pl.when(pl.program_id(0) == 0)
    def _():
        found = jnp.max(peaks[...], axis=0)
        for k, (out, least) in enumerate(((first_colmax, scale_floor), (second_colmax, 0.0))):
            wide = [found[k * half + at : k * half + at + 1] for at in range(half)]
            wide = jnp.maximum(jnp.concatenate(wide, axis=1), least)
            out[...] = wide
            inverse[k : k + 1, :] = 1.0 / wide

    for k, (values, by, out) in enumerate(
        ((first_new, by_first, first_scaled), (second_new, by_second, second_scaled))
    ):
        out[0] = values[...] * jnp.maximum(by[:, 0:1], inverse[k : k + 1, :])


def scaled_outputs(peaks, first_new, second_new, by_first, by_second):
    rows, cols = first_new.shape
    step = min(rows, 64)
    whole, side = pl.BlockSpec((step, cols), lambda r: (r, 0)), pl.BlockSpec((step, 128), lambda r: (r, 0))
    out, line = pl.BlockSpec((1, step, cols), lambda r: (0, r, 0)), pl.BlockSpec((1, cols), lambda r: (0, 0))
    big, wide = jax.ShapeDtypeStruct((1, rows, cols), F32), jax.ShapeDtypeStruct((1, cols), F32)
    return pl.pallas_call(
        scaled_body,
        grid=(rows // step,),
        out_shape=(big, big, wide, wide),
        in_specs=[pl.BlockSpec(memory_space=VMEM), whole, whole, side, side],
        out_specs=(out, out, line, line),
        scratch_shapes=[VMEM((8, cols), F32)],
        compiler_params=pltpu.CompilerParams(vmem_limit_bytes=VMEM_LIMIT),
        cost_estimate=pl.CostEstimate(flops=8 * rows * cols, bytes_accessed=16 * rows * cols, transcendentals=0),
        name="scaled_outputs",
    )(held(peaks), first_new, second_new, by_first, by_second)


def exchange(value, axes):
    return lax.all_to_all(value, axes, split_axis=0, concat_axis=0, tiled=True)


def local(
    grad_parts, first_codes, first_rows, first_columns, second_codes, second_rows, second_columns
):
    layer_count, _, row_count, col_count = grad_parts.shape
    entries = layer_count * lax.axis_size("section") * row_count * col_count
    devices, group = lax.axis_size(AXES), lax.axis_size(FSDP)
    parts = grad_parts.reshape(RING * RING, 2, 2, -1, col_count)
    old = (first_codes, first_rows, first_columns, second_codes, second_rows, second_columns)
    gradient, squares = reduce_scatter(parts, devices)
    squares = exchange(squares, AXES)
    first_old, second_old = old_moments(old)
    clip_limit = clip_rms * math.sqrt(entries)
    first_new, second_new, peaks = clip(squares, gradient, first_old, second_old, clip_limit, group)
    peaks = exchange(peaks, FSDP)
    direction, first_rowmax, second_rowmax, by_first, by_second = row_outputs(first_new, second_new)
    first_scaled, second_scaled, first_colmax, second_colmax = scaled_outputs(
        peaks, first_new, second_new, by_first, by_second
    )
    return (
        direction,
        first_scaled,
        second_scaled,
        first_rowmax,
        first_colmax,
        second_rowmax,
        second_colmax,
    )


def solution(mesh):
    torus = Mesh(mesh.devices.reshape(mesh.shape["section"], RING, RING, 2), AXES)
    placed = (
        P("section", FSDP, None, None),
        P("section", FSDP, None),
        P("section", FSDP),
        P("section", None),
        P("section", FSDP, None),
        P("section", FSDP),
        P("section", None),
    )
    return jax.shard_map(
        local,
        mesh=torus,
        in_specs=placed,
        out_specs=(
            P("section", FSDP, None),
            P("section", FSDP, None),
            P("section", FSDP, None),
            P("section", FSDP),
            P("section", None),
            P("section", FSDP),
            P("section", None),
        ),
        check_vma=False,
    )
```

```python
import functools
import math

import jax
import jax.numpy as jnp
from jax import lax
from jax.experimental import pallas as pl
from jax.experimental.pallas import tpu as pltpu
from jax.sharding import Mesh
from jax.sharding import PartitionSpec as P


AXES = ("section", "y", "z", "core")
FSDP = ("y", "z", "core")

beta_first = 0.9
beta_second = 0.999
clip_rms = 3.0
epsilon = 1e-08
scale_floor = 0.001

RING = 4
ORDER = (1, 3, 2, 0)
TOP = 32767.0
LEAST = 1e-18
SIDE = 8
STEP = 64
VMEM_LIMIT = 20 * 1024 * 1024
F32, I16 = jnp.float32, jnp.int16
VMEM = pltpu.VMEM


def scale_code(peak):
    return jnp.ceil(jnp.log2(jnp.maximum(peak, LEAST)) * 256.0)


def send_factor(code):
    return jnp.exp2(code * (-1.0 / 256.0)) * TOP**4


def encode(values, factor):
    root = lax.rsqrt(lax.rsqrt(jnp.abs(values) * factor))
    root = jnp.where(values < 0.0, -root, root)
    return jnp.round(root).astype(jnp.int32).astype(I16)


def came_factor(side):
    code = side[...].astype(jnp.int32).astype(F32)
    return jnp.exp2(code * (1.0 / 256.0)) * TOP**-4


def decode(codes, factor):
    root = codes.astype(jnp.int32).astype(F32)
    square = root * jnp.abs(root)
    return (square * jnp.abs(square)) * factor


def side_rows(codes):
    line = lax.broadcasted_iota(jnp.int32, (SIDE, codes[0].shape[1]), 0)
    rows = codes[-1]
    for at, code in enumerate(codes[:-1]):
        rows = jnp.where(line == at, code, rows)
    return jnp.broadcast_to(rows, line.shape).astype(jnp.int32).astype(I16)


def call(body, outs, scratch, flops, bytes_accessed, in_specs):
    return pl.pallas_call(
        body,
        out_shape=outs,
        in_specs=in_specs,
        out_specs=tuple(pl.BlockSpec(memory_space=VMEM) for _ in outs),
        scratch_shapes=scratch,
        compiler_params=pltpu.CompilerParams(vmem_limit_bytes=VMEM_LIMIT),
        cost_estimate=pl.CostEstimate(flops=flops, bytes_accessed=bytes_accessed, transcendentals=0),
    )


def in_vmem(n):
    return [pl.BlockSpec(memory_space=VMEM)] * n


def held(value):
    return pltpu.with_memory_space_constraint(value, VMEM)


def gather_copies(wanted, where, parts, outs, sem):
    copies = []
    for (jobs, mine), out in zip(wanted, outs):
        core = where[2] if mine else 1 - where[2]
        for q, (half, delta, low) in enumerate(jobs):
            for i in range(2):
                j = lax.rem(where[1 - half] + ORDER[low + i], RING)
                far = lax.rem(where[half] + delta, RING)
                at = far * RING + j if half == 0 else j * RING + far
                copies.append(
                    pltpu.make_async_copy(
                        parts.at[at, core, half], out.at[q, i], sem.at[len(copies)]
                    )
                )
    return copies


def gather_body(wanted, where, parts, *refs):
    copies = gather_copies(wanted, where, parts, refs[:-1], refs[-1])
    for copy in copies:
        copy.start()
    for copy in copies:
        copy.wait()


def gather_specs():
    return [pl.BlockSpec(memory_space=pltpu.SMEM), pl.BlockSpec(memory_space=pltpu.HBM)]


def gather_outs(parts, wanted):
    rows, cols = parts.shape[3:]
    return (
        tuple(VMEM((2, 2, rows, cols), parts.dtype) for _ in wanted),
        pltpu.SemaphoreType.DMA((4 * len(wanted),)),
        16 * len(wanted) * rows * cols,
    )


def gather(where, parts, wanted):
    outs, sem, moved = gather_outs(parts, wanted)
    body = functools.partial(gather_body, wanted)
    return call(body, outs, [sem], moved // 4, moved, gather_specs())(where, parts)


def chunks(rows, step, carry):
    return lax.fori_loop(0, rows // STEP, lambda n, c: step(pl.multiple_of(n * STEP, STEP), c), carry)


def fold(values, join):
    folded = values[0:8]
    for at in range(8, values.shape[0], 8):
        folded = join(folded, values[at : at + 8])
    return folded


def send_blocks(total, outs, peaks, rows, each):
    code = scale_code(jnp.concatenate(peaks, axis=0))
    factor = send_factor(code)
    for q, out in enumerate(outs):
        for i in range(each):
            line = q * each + i
            by = factor[line : line + 1]

            def step(r, _, line=line, by=by, out=out, i=i):
                out[pl.ds(i * rows + r, STEP), :] = encode(total[line, pl.ds(r, STEP), :], by)

            chunks(rows, step, None)
        out[each * rows : each * rows + SIDE, :] = side_rows(
            [code[q * each + i : q * each + i + 1] for i in range(each)]
        )


def pair_body(relays, wanted, *refs):
    own, came = refs[:2]
    relayed, refs = refs[2 : 2 + relays], refs[2 + relays :]
    copies = []
    if wanted:
        (where, parts), refs = refs[:2], refs[2:]
        copies = gather_copies(wanted, where, parts, refs[2 : 2 + len(wanted)], refs[-1])
    for copy in copies:
        copy.start()
    outs, total = refs[:2], refs[2 + len(wanted)]
    rows, cols = own.shape[2:]
    peaks = []
    for q in range(2):
        by = came_factor(relayed[q].at[2 * rows : 2 * rows + SIDE]) if relayed else None
        for i in range(2):

            def step(r, peak, q=q, i=i, by=by):
                value = own[q, i, pl.ds(r, STEP), :].astype(F32) + came[q, i, pl.ds(r, STEP), :].astype(F32)
                if relayed:
                    value = value + decode(relayed[q][pl.ds(i * rows + r, STEP), :], by[i : i + 1])
                total[2 * q + i, pl.ds(r, STEP), :] = value
                return jnp.maximum(peak, fold(jnp.abs(value), jnp.maximum))

            peak = chunks(rows, step, jnp.zeros((8, cols), F32))
            peaks.append(jnp.max(peak, axis=0, keepdims=True))
    send_blocks(total, outs, peaks, rows, 2)
    for copy in copies:
        copy.wait()


def pair(own, came, relayed=(), where=None, parts=None, wanted=()):
    rows, cols = own.shape[2:]
    outs, scratch = (VMEM((2 * rows + SIDE, cols), I16),) * 2, [VMEM((4, rows, cols), F32)]
    specs, args = in_vmem(2 + len(relayed)), [own, held(came), *[held(r) for r in relayed]]
    if wanted:
        more, sem, _ = gather_outs(parts, wanted)
        outs, scratch = outs + more, scratch + [sem]
        specs, args = specs + gather_specs(), args + [where, parts]
    got = call(
        functools.partial(pair_body, len(relayed), wanted), outs, scratch, 200 * rows * cols, 24 * rows * cols, specs
    )(*args)
    return got[:2], got[2:]


def column_of(row):
    n = row.shape[1]
    return jnp.transpose(jnp.broadcast_to(row, (128, n)))[:, 0:1]


def row_of(column):
    n = column.shape[0]
    return jnp.transpose(jnp.broadcast_to(column, (n, 128)))[0:1, :]


def keep_body(*refs):
    owns, cames, got, old = refs[:2], refs[2:4], refs[4:8], refs[8:14]
    total, first_old, second_old = refs[14:]
    rows = owns[0].shape[2]
    for half in range(2):
        for i in range(RING):
            ref = got[2 * half + (1 if i < 2 else 0)]
            by = came_factor(ref.at[2 * rows : 2 * rows + SIDE])[i % 2 : i % 2 + 1]

            def step(r, _, ref=ref, by=by, half=half, i=i, own=owns[half], came=cames[half]):
                at = (i // 2, i % 2, pl.ds(r, STEP))
                value = own[at].astype(F32) + came[at].astype(F32)
                total[half, i, pl.ds(r, STEP), :] = value + decode(ref[pl.ds(i % 2 * rows + r, STEP), :], by)

            chunks(rows, step, None)
    for (codes, row, column), levels, beta, out in (
        (old[:3], 7.0, beta_first, first_old),
        (old[3:], 15.0, beta_second, second_old),
    ):
        tall, wide = column_of(row[...]), column[...]
        for r in range(0, out.shape[0], STEP):
            bound = jnp.minimum(tall[r : r + STEP], wide)
            out[r : r + STEP, :] = codes[0, r : r + STEP, :].astype(F32) * (beta / levels) * bound


def keep(own, came, got, old):
    rows, cols = own[0].shape[2:]
    each = VMEM((2 * rows, cols), F32)
    return call(
        keep_body, (VMEM((2, RING, rows, cols), F32), each, each), [], 300 * rows * cols, 100 * rows * cols, in_vmem(14)
    )(*own, *[held(c) for c in came], *[held(g) for g in got], *old)


def middle_body(half, acc, first, second, *refs):
    outs, kept, total = refs[:3], refs[3], refs[4]
    rows, cols = kept.shape
    peaks = []
    for i in range(RING):
        ref = first if i < 2 else second
        by = came_factor(ref.at[2 * rows : 2 * rows + SIDE])[i % 2 : i % 2 + 1]

        def step(r, peak, ref=ref, by=by, i=i):
            value = acc[half, i, pl.ds(r, STEP), :] + decode(ref[pl.ds(i % 2 * rows + r, STEP), :], by)
            if i == 3:
                kept[pl.ds(r, STEP), :] = value
                return peak
            total[i, pl.ds(r, STEP), :] = value
            return jnp.maximum(peak, fold(jnp.abs(value), jnp.maximum))

        peak = chunks(rows, step, jnp.zeros((8, cols), F32))
        if i < 3:
            peaks.append(jnp.max(peak, axis=0, keepdims=True))
    send_blocks(total, outs, peaks, rows, 1)


def middle(acc, first, second, half):
    rows, cols = acc.shape[2:]
    sent = VMEM((rows + SIDE, cols), I16)
    return call(
        functools.partial(middle_body, half),
        (sent, sent, sent, VMEM((rows, cols), F32)),
        [VMEM((3, rows, cols), F32)],
        200 * rows * cols,
        32 * rows * cols,
        in_vmem(3),
    )(acc, held(first), held(second))


def last_body(*refs):
    ins, (grad, squares) = refs[:8], refs[8:]
    rows, cols = ins[0].shape
    square = jnp.zeros((8, cols), F32)
    for half in range(2):
        kept, *got = ins[4 * half : 4 * half + 4]
        by = [came_factor(ref.at[rows : rows + SIDE])[0:1] for ref in got]

        def step(r, square, half=half, kept=kept, got=got, by=by):
            value = kept[pl.ds(r, STEP), :]
            for ref, factor in zip(got, by):
                value = value + decode(ref[pl.ds(r, STEP), :], factor)
            grad[pl.ds(half * rows + r, STEP), :] = value
            return square + fold(value * value, jnp.add)

        square = chunks(rows, step, square)
    folded = square[:, 0:128]
    for at in range(128, cols, 128):
        folded = folded + square[:, at : at + 128]
    squares[...] = jnp.broadcast_to(jnp.sum(folded, axis=0, keepdims=True), squares.shape)


def last(halves, devices):
    rows, cols = halves[0][0].shape
    flat = [a for kept, *got in halves for a in (kept, *[held(g) for g in got])]
    return call(
        last_body,
        (VMEM((2 * rows, cols), F32), VMEM((devices, 128), F32)),
        [],
        100 * rows * cols,
        32 * rows * cols,
        in_vmem(8),
    )(*flat)


def reduce_scatter(parts, old, devices):
    where = jnp.stack([lax.axis_index(a) for a in FSDP]).astype(jnp.int32)
    parts = pltpu.with_memory_space_constraint(parts, pltpu.HBM)
    axis = ("y", "z")

    def hop(value, name, delta):
        return lax.ppermute(value, name, [(i, (i + delta) % RING) for i in range(RING)])

    def swap(value):
        return lax.ppermute(value, "core", [(0, 1), (1, 0)])

    def stage(half, own, came, relayed, wanted):
        sent, more = pair(own, came, relayed, where, parts, wanted)
        got = []
        for value, delta in zip(sent, (1, 3)):
            got.append(hop(value, axis[half], delta))
        return got, more

    def jobs(half, *each):
        return tuple((half, delta, low) for delta, low in each)

    far, near, join, mine = (
        [jobs(half, *each) for half in range(2)]
        for each in (((2, 0), (2, 2)), ((1, 2), (3, 0)), ((1, 0), (3, 2)), ((0, 0), (0, 2)))
    )
    (out,) = gather(where, parts, ((far[0], False),))
    came_far_0 = swap(out)
    out, own_far_0 = gather(where, parts, ((far[1], False), (far[0], True)))
    came_far_1 = swap(out)
    far_0, (out, own_far_1) = stage(0, own_far_0, came_far_0, (), ((near[0], False), (far[1], True)))
    came_near_0 = swap(out)
    far_1, (out, own_near_0) = stage(1, own_far_1, came_far_1, (), ((near[1], False), (near[0], True)))
    came_near_1 = swap(out)
    near_0, (out, own_near_1) = stage(0, own_near_0, came_near_0, (), ((join[0], False), (near[1], True)))
    came_join_0 = swap(out)
    near_1, (out, own_join_0) = stage(1, own_near_1, came_near_1, (), ((join[1], False), (join[0], True)))
    came_join_1 = swap(out)
    join_0, (out, own_join_1) = stage(0, own_join_0, came_join_0, far_0, ((mine[0], False), (join[1], True)))
    came_mine_0 = swap(out)
    join_1, (out, own_mine_0, own_mine_1) = stage(
        1, own_join_1, came_join_1, far_1, ((mine[1], False), (mine[0], True), (mine[1], True))
    )
    came_mine_1 = swap(out)
    acc, first_old, second_old = keep(
        (own_mine_0, own_mine_1), (came_mine_0, came_mine_1), (*near_0, *near_1), old
    )
    halves = []
    for half, joined in enumerate((join_0, join_1)):
        *out, kept = middle(acc, *joined, half)
        got = []
        for k, delta in ((2, 2), (0, 1), (1, 3)):
            got.append(hop(out[k], axis[1 - half], delta))
        halves.append([kept] + got)
    return *last(halves, devices), first_old, second_old


def clip_body(limit, squares, grad, first_old, second_old, first_new, second_new, peaks):
    rows, cols = grad.shape
    total = jnp.sum(jnp.sum(squares[...], axis=0, keepdims=True), axis=1, keepdims=True)
    scale = limit / jnp.maximum(jnp.sqrt(total), limit)

    def step(r, peak):
        clipped = grad[pl.ds(r, STEP), :] * scale
        first = first_old[pl.ds(r, STEP), :] + (1.0 - beta_first) * clipped
        second = second_old[pl.ds(r, STEP), :] + (1.0 - beta_second) * clipped * clipped
        first_new[pl.ds(r, STEP), :] = first
        second_new[pl.ds(r, STEP), :] = second
        return (
            jnp.maximum(peak[0], fold(jnp.abs(first), jnp.maximum)),
            jnp.maximum(peak[1], fold(second, jnp.maximum)),
        )

    zero = jnp.zeros((8, cols), F32)
    found = chunks(rows, step, (zero, zero))
    lines = []
    for peak in found:
        peak = jnp.max(peak, axis=0, keepdims=True)
        lines += [peak[:, at : at + 128] for at in range(0, cols, 128)]
    lines = jnp.concatenate(lines, axis=0)
    for at in range(peaks.shape[0]):
        peaks[at] = lines


def clip(squares, grad, first_old, second_old, limit, group):
    rows, cols = grad.shape
    each = VMEM((rows, cols), F32)
    return call(
        functools.partial(clip_body, limit),
        (each, each, VMEM((group, 2 * cols // 128, 128), F32)),
        [],
        12 * rows * cols,
        20 * rows * cols,
        in_vmem(4),
    )(held(squares), grad, first_old, second_old)


def rows_body(first_new, second_new, direction, first_rowmax, second_rowmax, by_first, by_second):
    first, second = first_new[...], second_new[...]
    direction[0] = first / (jnp.sqrt(second) + epsilon)
    for values, least, peak, by in (
        (jnp.abs(first), scale_floor, first_rowmax, by_first),
        (second, 0.0, second_rowmax, by_second),
    ):
        tall = jnp.maximum(jnp.max(values, axis=1, keepdims=True), least)
        by[...] = jnp.broadcast_to(1.0 / tall, by.shape)
        peak[...] = row_of(tall)


def row_outputs(first_new, second_new):
    rows, cols = first_new.shape
    step = min(rows, 128)
    whole = pl.BlockSpec((step, cols), lambda r: (r, 0))
    side, line = pl.BlockSpec((step, 128), lambda r: (r, 0)), pl.BlockSpec((1, step), lambda r: (0, r))
    return pl.pallas_call(
        rows_body,
        grid=(rows // step,),
        out_shape=(
            jax.ShapeDtypeStruct((1, rows, cols), F32),
            jax.ShapeDtypeStruct((1, rows), F32),
            jax.ShapeDtypeStruct((1, rows), F32),
            VMEM((rows, 128), F32),
            VMEM((rows, 128), F32),
        ),
        in_specs=[whole, whole],
        out_specs=(pl.BlockSpec((1, step, cols), lambda r: (0, r, 0)), line, line, side, side),
        compiler_params=pltpu.CompilerParams(vmem_limit_bytes=VMEM_LIMIT),
        cost_estimate=pl.CostEstimate(flops=40 * rows * cols, bytes_accessed=12 * rows * cols, transcendentals=0),
        name="row_outputs",
    )(first_new, second_new)


def scaled_body(peaks, first_new, second_new, by_first, by_second, *refs):
    first_scaled, second_scaled, first_colmax, second_colmax, inverse = refs
    half = peaks.shape[1] // 2

    @pl.when(pl.program_id(0) == 0)
    def _():
        found = jnp.max(peaks[...], axis=0)
        for k, (out, least) in enumerate(((first_colmax, scale_floor), (second_colmax, 0.0))):
            wide = [found[k * half + at : k * half + at + 1] for at in range(half)]
            wide = jnp.maximum(jnp.concatenate(wide, axis=1), least)
            out[...] = wide
            inverse[k : k + 1, :] = 1.0 / wide

    for k, (values, by, out) in enumerate(
        ((first_new, by_first, first_scaled), (second_new, by_second, second_scaled))
    ):
        out[0] = values[...] * jnp.maximum(by[:, 0:1], inverse[k : k + 1, :])


def scaled_outputs(peaks, first_new, second_new, by_first, by_second):
    rows, cols = first_new.shape
    step = min(rows, 64)
    whole, side = pl.BlockSpec((step, cols), lambda r: (r, 0)), pl.BlockSpec((step, 128), lambda r: (r, 0))
    out, line = pl.BlockSpec((1, step, cols), lambda r: (0, r, 0)), pl.BlockSpec((1, cols), lambda r: (0, 0))
    big, wide = jax.ShapeDtypeStruct((1, rows, cols), F32), jax.ShapeDtypeStruct((1, cols), F32)
    return pl.pallas_call(
        scaled_body,
        grid=(rows // step,),
        out_shape=(big, big, wide, wide),
        in_specs=[pl.BlockSpec(memory_space=VMEM), whole, whole, side, side],
        out_specs=(out, out, line, line),
        scratch_shapes=[VMEM((8, cols), F32)],
        compiler_params=pltpu.CompilerParams(vmem_limit_bytes=VMEM_LIMIT),
        cost_estimate=pl.CostEstimate(flops=8 * rows * cols, bytes_accessed=16 * rows * cols, transcendentals=0),
        name="scaled_outputs",
    )(held(peaks), first_new, second_new, by_first, by_second)


def exchange(value, axes):
    return lax.all_to_all(value, axes, split_axis=0, concat_axis=0, tiled=True)


def local(
    grad_parts, first_codes, first_rows, first_columns, second_codes, second_rows, second_columns
):
    layer_count, _, row_count, col_count = grad_parts.shape
    entries = layer_count * lax.axis_size("section") * row_count * col_count
    devices, group = lax.axis_size(AXES), lax.axis_size(FSDP)
    parts = grad_parts.reshape(RING * RING, 2, 2, -1, col_count)
    old = (first_codes, first_rows, first_columns, second_codes, second_rows, second_columns)
    gradient, squares, first_old, second_old = reduce_scatter(parts, old, devices)
    squares = exchange(squares, AXES)
    clip_limit = clip_rms * math.sqrt(entries)
    first_new, second_new, peaks = clip(squares, gradient, first_old, second_old, clip_limit, group)
    peaks = exchange(peaks, FSDP)
    direction, first_rowmax, second_rowmax, by_first, by_second = row_outputs(first_new, second_new)
    first_scaled, second_scaled, first_colmax, second_colmax = scaled_outputs(
        peaks, first_new, second_new, by_first, by_second
    )
    return (
        direction,
        first_scaled,
        second_scaled,
        first_rowmax,
        first_colmax,
        second_rowmax,
        second_colmax,
    )


def solution(mesh):
    torus = Mesh(mesh.devices.reshape(mesh.shape["section"], RING, RING, 2), AXES)
    placed = (
        P("section", FSDP, None, None),
        P("section", FSDP, None),
        P("section", FSDP),
        P("section", None),
        P("section", FSDP, None),
        P("section", FSDP),
        P("section", None),
    )
    return jax.shard_map(
        local,
        mesh=torus,
        in_specs=placed,
        out_specs=(
            P("section", FSDP, None),
            P("section", FSDP, None),
            P("section", FSDP, None),
            P("section", FSDP),
            P("section", None),
            P("section", FSDP),
            P("section", None),
        ),
        check_vma=False,
    )
```

```python
import functools
import math

import jax
import jax.numpy as jnp
from jax import lax
from jax.experimental import pallas as pl
from jax.experimental.pallas import tpu as pltpu
from jax.sharding import Mesh
from jax.sharding import PartitionSpec as P


AXES = ("section", "y", "z", "core")
FSDP = ("y", "z", "core")

beta_first = 0.9
beta_second = 0.999
clip_rms = 3.0
epsilon = 1e-08
scale_floor = 0.001

RING = 4
ORDER = (1, 3, 2, 0)
TOP = 32767.0
LEAST = 1e-18
SIDE = 8
STEP = 64
VMEM_LIMIT = 8 * 1024 * 1024
F32, I16 = jnp.float32, jnp.int16
VMEM = pltpu.VMEM


def scale_code(peak):
    return jnp.ceil(jnp.log2(jnp.maximum(peak, LEAST)) * 256.0)


def send_factor(code):
    return jnp.exp2(code * (-1.0 / 256.0)) * TOP**4


def encode(values, factor):
    root = lax.rsqrt(lax.rsqrt(jnp.abs(values) * factor))
    root = jnp.where(values < 0.0, -root, root)
    return jnp.round(root).astype(jnp.int32).astype(I16)


def came_factor(side):
    code = side[...].astype(jnp.int32).astype(F32)
    return jnp.exp2(code * (1.0 / 256.0)) * TOP**-4


def decode(codes, factor):
    root = codes.astype(jnp.int32).astype(F32)
    square = root * jnp.abs(root)
    return (square * jnp.abs(square)) * factor


def side_rows(codes):
    line = lax.broadcasted_iota(jnp.int32, (SIDE, codes[0].shape[1]), 0)
    rows = codes[-1]
    for at, code in enumerate(codes[:-1]):
        rows = jnp.where(line == at, code, rows)
    return jnp.broadcast_to(rows, line.shape).astype(jnp.int32).astype(I16)


def call(body, outs, scratch, flops, bytes_accessed, in_specs):
    return pl.pallas_call(
        body,
        out_shape=outs,
        in_specs=in_specs,
        out_specs=tuple(pl.BlockSpec(memory_space=VMEM) for _ in outs),
        scratch_shapes=scratch,
        compiler_params=pltpu.CompilerParams(vmem_limit_bytes=VMEM_LIMIT),
        cost_estimate=pl.CostEstimate(flops=flops, bytes_accessed=bytes_accessed, transcendentals=0),
    )


def in_vmem(n):
    return [pl.BlockSpec(memory_space=VMEM)] * n


def held(value):
    return pltpu.with_memory_space_constraint(value, VMEM)


def block_at(where, job, i):
    half, delta, low = job
    j = lax.rem(where[1 - half] + ORDER[low + i], RING)
    far = lax.rem(where[half] + delta, RING)
    return far * RING + j if half == 0 else j * RING + far


def gather_body(wanted, where, parts, *refs):
    outs, sem = refs[:-1], refs[-1]
    copies = []
    for (jobs, mine), out in zip(wanted, outs):
        core = where[2] if mine else 1 - where[2]
        for q, job in enumerate(jobs):
            for i in range(2):
                source = parts.at[block_at(where, job, i), core, job[0]]
                copies.append(pltpu.make_async_copy(source, out.at[q, i], sem.at[len(copies)]))
    for copy in copies:
        copy.start()
    for copy in copies:
        copy.wait()


def gather(where, parts, wanted):
    rows, cols = parts.shape[3:]
    size = 2 * rows * cols * sum(len(jobs) for jobs, _ in wanted)
    return call(
        functools.partial(gather_body, wanted),
        tuple(VMEM((len(jobs), 2, rows, cols), parts.dtype) for jobs, _ in wanted),
        [pltpu.SemaphoreType.DMA((2 * sum(len(jobs) for jobs, _ in wanted),))],
        size,
        4 * size,
        [pl.BlockSpec(memory_space=pltpu.SMEM), pl.BlockSpec(memory_space=pltpu.HBM)],
    )(where, pltpu.with_memory_space_constraint(parts, pltpu.HBM))


def chunks(rows, step, carry):
    return lax.fori_loop(0, rows // STEP, lambda n, c: step(pl.multiple_of(n * STEP, STEP), c), carry)


def fold(values, join):
    folded = values[0:8]
    for at in range(8, values.shape[0], 8):
        folded = join(folded, values[at : at + 8])
    return folded


def send_blocks(total, outs, peaks, rows, each):
    code = scale_code(jnp.concatenate(peaks, axis=0))
    factor = send_factor(code)
    for q, out in enumerate(outs):
        for i in range(each):
            line = q * each + i
            by = factor[line : line + 1]

            def step(r, _, line=line, by=by, out=out, i=i):
                out[pl.ds(i * rows + r, STEP), :] = encode(total[line, pl.ds(r, STEP), :], by)

            chunks(rows, step, None)
        out[each * rows : each * rows + SIDE, :] = side_rows(
            [code[q * each + i : q * each + i + 1] for i in range(each)]
        )


def pair_body(jobs, at_came, first, relays, sends, *refs):
    (where, parts, came), refs = refs[:3], refs[3:]
    relayed, refs = refs[:relays], refs[relays:]
    outs, total = refs[: len(jobs)], refs[-1]
    rows, cols = came.shape[2:]
    core = where[2]
    for out, wanted in zip(refs[len(jobs) : -1], sends):
        for q, job in enumerate(wanted):
            for i in range(2):
                at = block_at(where, job, i)
                for r in range(0, rows, STEP):
                    out[q, i, r : r + STEP, :] = parts[at, 1 - core, job[0], r : r + STEP, :]
    peaks = []
    for q, job in enumerate(jobs):
        by = came_factor(relayed[q].at[2 * rows : 2 * rows + SIDE]) if relayed else None
        for i in range(2):
            at = (q, i) if first else (block_at(where, job, i), core, job[0])

            def step(r, peak, q=q, i=i, by=by, at=at):
                value = parts[(*at, pl.ds(r, STEP))].astype(F32) + came[at_came + q, i, pl.ds(r, STEP), :].astype(F32)
                if relayed:
                    value = value + decode(relayed[q][pl.ds(i * rows + r, STEP), :], by[i : i + 1])
                total[2 * q + i, pl.ds(r, STEP), :] = value
                return jnp.maximum(peak, fold(jnp.abs(value), jnp.maximum))

            peak = chunks(rows, step, jnp.zeros((8, cols), F32))
            peaks.append(jnp.max(peak, axis=0, keepdims=True))
    send_blocks(total, outs, peaks, rows, 2)


def pair(where, parts, came, jobs, first=False, relayed=(), sends=()):
    rows, cols = came.shape[2:]
    at_came = len(jobs) * jobs[0][0] if came.shape[0] > len(jobs) else 0
    got = call(
        functools.partial(pair_body, jobs, at_came, first, len(relayed), sends),
        (VMEM((2 * rows + SIDE, cols), I16),) * len(jobs)
        + tuple(VMEM((len(wanted), 2, rows, cols), came.dtype) for wanted in sends),
        [VMEM((2 * len(jobs), rows, cols), F32)],
        100 * len(jobs) * rows * cols,
        12 * len(jobs) * rows * cols,
        [pl.BlockSpec(memory_space=pltpu.SMEM), *in_vmem(2 + len(relayed))],
    )(where, parts, held(came), *[held(r) for r in relayed])
    return got[: len(jobs)], got[len(jobs) :]


def column_of(row):
    n = row.shape[1]
    return jnp.transpose(jnp.broadcast_to(row, (128, n)))[:, 0:1]


def row_of(column):
    n = column.shape[0]
    return jnp.transpose(jnp.broadcast_to(column, (n, 128)))[0:1, :]


def keep_body(jobs, where, parts, came, *refs):
    got, old = refs[:4], refs[4:10]
    total, first_old, second_old = refs[10:]
    rows = came.shape[2]
    for half in range(2):
        for i in range(RING):
            ref = got[2 * half + (1 if i < 2 else 0)]
            by = came_factor(ref.at[2 * rows : 2 * rows + SIDE])[i % 2 : i % 2 + 1]
            q = 2 * half + i // 2
            at = (block_at(where, jobs[q], i % 2), where[2], half)

            def step(r, _, ref=ref, by=by, half=half, i=i, q=q, at=at):
                value = parts[(*at, pl.ds(r, STEP))].astype(F32) + came[q, i % 2, pl.ds(r, STEP), :].astype(F32)
                total[half, i, pl.ds(r, STEP), :] = value + decode(ref[pl.ds(i % 2 * rows + r, STEP), :], by)

            chunks(rows, step, None)
    for (codes, row, column), levels, beta, out in (
        (old[:3], 7.0, beta_first, first_old),
        (old[3:], 15.0, beta_second, second_old),
    ):
        tall, wide = column_of(row[...]), column[...]
        for r in range(0, out.shape[0], STEP):
            bound = jnp.minimum(tall[r : r + STEP], wide)
            out[r : r + STEP, :] = codes[0, r : r + STEP, :].astype(F32) * (beta / levels) * bound


def keep(where, parts, came, jobs, got, old):
    rows, cols = came.shape[2:]
    each = VMEM((2 * rows, cols), F32)
    return call(
        functools.partial(keep_body, jobs),
        (VMEM((2, RING, rows, cols), F32), each, each),
        [],
        300 * rows * cols,
        100 * rows * cols,
        [pl.BlockSpec(memory_space=pltpu.SMEM), *in_vmem(12)],
    )(where, parts, held(came), *[held(g) for g in got], *old)


def middle_body(half, acc, first, second, *refs):
    outs, kept, total = refs[:3], refs[3], refs[4]
    rows, cols = kept.shape
    peaks = []
    for i in range(RING):
        ref = first if i < 2 else second
        by = came_factor(ref.at[2 * rows : 2 * rows + SIDE])[i % 2 : i % 2 + 1]

        def step(r, peak, ref=ref, by=by, i=i):
            value = acc[half, i, pl.ds(r, STEP), :] + decode(ref[pl.ds(i % 2 * rows + r, STEP), :], by)
            if i == 3:
                kept[pl.ds(r, STEP), :] = value
                return peak
            total[i, pl.ds(r, STEP), :] = value
            return jnp.maximum(peak, fold(jnp.abs(value), jnp.maximum))

        peak = chunks(rows, step, jnp.zeros((8, cols), F32))
        if i < 3:
            peaks.append(jnp.max(peak, axis=0, keepdims=True))
    send_blocks(total, outs, peaks, rows, 1)


def middle(acc, first, second, half):
    rows, cols = acc.shape[2:]
    sent = VMEM((rows + SIDE, cols), I16)
    return call(
        functools.partial(middle_body, half),
        (sent, sent, sent, VMEM((rows, cols), F32)),
        [VMEM((3, rows, cols), F32)],
        200 * rows * cols,
        32 * rows * cols,
        in_vmem(3),
    )(acc, held(first), held(second))


def last_body(*refs):
    ins, (grad, squares) = refs[:8], refs[8:]
    rows, cols = ins[0].shape
    square = jnp.zeros((8, cols), F32)
    for half in range(2):
        kept, *got = ins[4 * half : 4 * half + 4]
        by = [came_factor(ref.at[rows : rows + SIDE])[0:1] for ref in got]

        def step(r, square, half=half, kept=kept, got=got, by=by):
            value = kept[pl.ds(r, STEP), :]
            for ref, factor in zip(got, by):
                value = value + decode(ref[pl.ds(r, STEP), :], factor)
            grad[pl.ds(half * rows + r, STEP), :] = value
            return square + fold(value * value, jnp.add)

        square = chunks(rows, step, square)
    folded = square[:, 0:128]
    for at in range(128, cols, 128):
        folded = folded + square[:, at : at + 128]
    squares[...] = jnp.broadcast_to(jnp.sum(folded, axis=0, keepdims=True), squares.shape)


def last(halves, devices):
    rows, cols = halves[0][0].shape
    flat = [a for kept, *got in halves for a in (kept, *[held(g) for g in got])]
    return call(
        last_body,
        (VMEM((2 * rows, cols), F32), VMEM((devices, 128), F32)),
        [],
        100 * rows * cols,
        32 * rows * cols,
        in_vmem(8),
    )(*flat)


def reduce_scatter(parts, old, devices):
    where = jnp.stack([lax.axis_index(a) for a in FSDP]).astype(jnp.int32)
    resident = held(parts)
    axis = ("y", "z")

    def hop(value, name, delta):
        return lax.ppermute(value, name, [(i, (i + delta) % RING) for i in range(RING)])

    def swap(value):
        return lax.ppermute(value, "core", [(0, 1), (1, 0)])

    def stage(half, jobs, came, source=resident, first=False, relayed=(), sends=()):
        sent, more = pair(where, source, came, jobs, first, relayed, sends)
        got = []
        for value, delta in zip(sent, (1, 3)):
            got.append(hop(value, axis[half], delta))
        return got, more

    def jobs_of(*each):
        return [tuple((half, delta, low) for delta, low in each) for half in range(2)]

    far, near = jobs_of((2, 0), (2, 2)), jobs_of((1, 2), (3, 0))
    join, mine = jobs_of((1, 0), (3, 2)), jobs_of((0, 0), (0, 2))
    (out,) = gather(where, parts, ((far[0], False),))
    came_far_0 = swap(out)
    out, own_far_0 = gather(where, parts, ((far[1], False), (far[0], True)))
    came_far_1 = swap(out)
    far_0, _ = stage(0, far[0], came_far_0, own_far_0, True)
    far_1, out = stage(1, far[1], came_far_1, sends=near)
    came_near = [swap(o) for o in out]
    near_0, (out,) = stage(0, near[0], came_near[0], sends=(join[0] + join[1],))
    came_join = swap(out)
    near_1, (out,) = stage(1, near[1], came_near[1], sends=(mine[0] + mine[1],))
    came_mine = swap(out)
    join_0, _ = stage(0, join[0], came_join, relayed=far_0)
    join_1, _ = stage(1, join[1], came_join, relayed=far_1)
    acc, first_old, second_old = keep(
        where, resident, came_mine, mine[0] + mine[1], (*near_0, *near_1), old
    )
    halves = []
    for half, joined in enumerate((join_0, join_1)):
        *out, kept = middle(acc, *joined, half)
        got = []
        for k, delta in ((2, 2), (0, 1), (1, 3)):
            got.append(hop(out[k], axis[1 - half], delta))
        halves.append([kept] + got)
    return *last(halves, devices), first_old, second_old


def clip_body(limit, squares, grad, first_old, second_old, first_new, second_new, peaks):
    rows, cols = grad.shape
    total = jnp.sum(jnp.sum(squares[...], axis=0, keepdims=True), axis=1, keepdims=True)
    scale = limit / jnp.maximum(jnp.sqrt(total), limit)

    def step(r, peak):
        clipped = grad[pl.ds(r, STEP), :] * scale
        first = first_old[pl.ds(r, STEP), :] + (1.0 - beta_first) * clipped
        second = second_old[pl.ds(r, STEP), :] + (1.0 - beta_second) * clipped * clipped
        first_new[pl.ds(r, STEP), :] = first
        second_new[pl.ds(r, STEP), :] = second
        return (
            jnp.maximum(peak[0], fold(jnp.abs(first), jnp.maximum)),
            jnp.maximum(peak[1], fold(second, jnp.maximum)),
        )

    zero = jnp.zeros((8, cols), F32)
    found = chunks(rows, step, (zero, zero))
    lines = []
    for peak in found:
        peak = jnp.max(peak, axis=0, keepdims=True)
        lines += [peak[:, at : at + 128] for at in range(0, cols, 128)]
    lines = jnp.concatenate(lines, axis=0)
    for at in range(peaks.shape[0]):
        peaks[at] = lines


def clip(squares, grad, first_old, second_old, limit, group):
    rows, cols = grad.shape
    each = VMEM((rows, cols), F32)
    return call(
        functools.partial(clip_body, limit),
        (each, each, VMEM((group, 2 * cols // 128, 128), F32)),
        [],
        12 * rows * cols,
        20 * rows * cols,
        in_vmem(4),
    )(held(squares), grad, first_old, second_old)


def rows_body(first_new, second_new, direction, first_rowmax, second_rowmax, by_first, by_second):
    first, second = first_new[...], second_new[...]
    direction[0] = first / (jnp.sqrt(second) + epsilon)
    for values, least, peak, by in (
        (jnp.abs(first), scale_floor, first_rowmax, by_first),
        (second, 0.0, second_rowmax, by_second),
    ):
        tall = jnp.maximum(jnp.max(values, axis=1, keepdims=True), least)
        by[...] = jnp.broadcast_to(1.0 / tall, by.shape)
        peak[...] = row_of(tall)


def row_outputs(first_new, second_new):
    rows, cols = first_new.shape
    step = min(rows, 128)
    whole = pl.BlockSpec((step, cols), lambda r: (r, 0))
    side, line = pl.BlockSpec((step, 128), lambda r: (r, 0)), pl.BlockSpec((1, step), lambda r: (0, r))
    return pl.pallas_call(
        rows_body,
        grid=(rows // step,),
        out_shape=(
            jax.ShapeDtypeStruct((1, rows, cols), F32),
            jax.ShapeDtypeStruct((1, rows), F32),
            jax.ShapeDtypeStruct((1, rows), F32),
            VMEM((rows, 128), F32),
            VMEM((rows, 128), F32),
        ),
        in_specs=[whole, whole],
        out_specs=(pl.BlockSpec((1, step, cols), lambda r: (0, r, 0)), line, line, side, side),
        compiler_params=pltpu.CompilerParams(vmem_limit_bytes=VMEM_LIMIT),
        cost_estimate=pl.CostEstimate(flops=40 * rows * cols, bytes_accessed=12 * rows * cols, transcendentals=0),
        name="row_outputs",
    )(first_new, second_new)


def scaled_body(peaks, first_new, second_new, by_first, by_second, *refs):
    first_scaled, second_scaled, first_colmax, second_colmax, inverse = refs
    half = peaks.shape[1] // 2

    @pl.when(pl.program_id(0) == 0)
    def _():
        found = jnp.max(peaks[...], axis=0)
        for k, (out, least) in enumerate(((first_colmax, scale_floor), (second_colmax, 0.0))):
            wide = [found[k * half + at : k * half + at + 1] for at in range(half)]
            wide = jnp.maximum(jnp.concatenate(wide, axis=1), least)
            out[...] = wide
            inverse[k : k + 1, :] = 1.0 / wide

    for k, (values, by, out) in enumerate(
        ((first_new, by_first, first_scaled), (second_new, by_second, second_scaled))
    ):
        out[0] = values[...] * jnp.maximum(by[:, 0:1], inverse[k : k + 1, :])


def scaled_outputs(peaks, first_new, second_new, by_first, by_second):
    rows, cols = first_new.shape
    step = min(rows, 64)
    whole, side = pl.BlockSpec((step, cols), lambda r: (r, 0)), pl.BlockSpec((step, 128), lambda r: (r, 0))
    out, line = pl.BlockSpec((1, step, cols), lambda r: (0, r, 0)), pl.BlockSpec((1, cols), lambda r: (0, 0))
    big, wide = jax.ShapeDtypeStruct((1, rows, cols), F32), jax.ShapeDtypeStruct((1, cols), F32)
    return pl.pallas_call(
        scaled_body,
        grid=(rows // step,),
        out_shape=(big, big, wide, wide),
        in_specs=[pl.BlockSpec(memory_space=VMEM), whole, whole, side, side],
        out_specs=(out, out, line, line),
        scratch_shapes=[VMEM((8, cols), F32)],
        compiler_params=pltpu.CompilerParams(vmem_limit_bytes=VMEM_LIMIT),
        cost_estimate=pl.CostEstimate(flops=8 * rows * cols, bytes_accessed=16 * rows * cols, transcendentals=0),
        name="scaled_outputs",
    )(held(peaks), first_new, second_new, by_first, by_second)


def exchange(value, axes):
    return lax.all_to_all(value, axes, split_axis=0, concat_axis=0, tiled=True)


def local(
    grad_parts, first_codes, first_rows, first_columns, second_codes, second_rows, second_columns
):
    layer_count, _, row_count, col_count = grad_parts.shape
    entries = layer_count * lax.axis_size("section") * row_count * col_count
    devices, group = lax.axis_size(AXES), lax.axis_size(FSDP)
    parts = grad_parts.reshape(RING * RING, 2, 2, -1, col_count)
    old = (first_codes, first_rows, first_columns, second_codes, second_rows, second_columns)
    gradient, squares, first_old, second_old = reduce_scatter(parts, old, devices)
    squares = exchange(squares, AXES)
    clip_limit = clip_rms * math.sqrt(entries)
    first_new, second_new, peaks = clip(squares, gradient, first_old, second_old, clip_limit, group)
    peaks = exchange(peaks, FSDP)
    direction, first_rowmax, second_rowmax, by_first, by_second = row_outputs(first_new, second_new)
    first_scaled, second_scaled, first_colmax, second_colmax = scaled_outputs(
        peaks, first_new, second_new, by_first, by_second
    )
    return (
        direction,
        first_scaled,
        second_scaled,
        first_rowmax,
        first_colmax,
        second_rowmax,
        second_colmax,
    )


def solution(mesh):
    torus = Mesh(mesh.devices.reshape(mesh.shape["section"], RING, RING, 2), AXES)
    placed = (
        P("section", FSDP, None, None),
        P("section", FSDP, None),
        P("section", FSDP),
        P("section", None),
        P("section", FSDP, None),
        P("section", FSDP),
        P("section", None),
    )
    return jax.shard_map(
        local,
        mesh=torus,
        in_specs=placed,
        out_specs=(
            P("section", FSDP, None),
            P("section", FSDP, None),
            P("section", FSDP, None),
            P("section", FSDP),
            P("section", None),
            P("section", FSDP),
            P("section", None),
        ),
        check_vma=False,
    )
```

```python
import functools
import math

import jax
import jax.numpy as jnp
from jax import lax
from jax.experimental import pallas as pl
from jax.experimental.pallas import tpu as pltpu
from jax.sharding import Mesh
from jax.sharding import PartitionSpec as P


AXES = ("section", "y", "z", "core")
FSDP = ("y", "z", "core")

beta_first = 0.9
beta_second = 0.999
clip_rms = 3.0
epsilon = 1e-08
scale_floor = 0.001

RING = 4
ORDER = (1, 3, 2, 0)
TOP = 32767.0
LEAST = 1e-18
SIDE = 8
STEP = 64
VMEM_LIMIT = 8 * 1024 * 1024
F32, I16 = jnp.float32, jnp.int16
VMEM = pltpu.VMEM


def scale_code(peak):
    return jnp.ceil(jnp.log2(jnp.maximum(peak, LEAST)) * 256.0)


def send_factor(code):
    return jnp.exp2(code * (-1.0 / 256.0)) * TOP**4


def encode(values, factor):
    root = lax.rsqrt(lax.rsqrt(jnp.abs(values) * factor))
    root = jnp.where(values < 0.0, -root, root)
    return jnp.round(root).astype(jnp.int32).astype(I16)


def came_factor(side):
    code = side[...].astype(jnp.int32).astype(F32)
    return jnp.exp2(code * (1.0 / 256.0)) * TOP**-4


def decode(codes, factor):
    root = codes.astype(jnp.int32).astype(F32)
    square = root * jnp.abs(root)
    return (square * jnp.abs(square)) * factor


def side_rows(codes):
    line = lax.broadcasted_iota(jnp.int32, (SIDE, codes[0].shape[1]), 0)
    rows = codes[-1]
    for at, code in enumerate(codes[:-1]):
        rows = jnp.where(line == at, code, rows)
    return jnp.broadcast_to(rows, line.shape).astype(jnp.int32).astype(I16)


def call(body, outs, scratch, flops, bytes_accessed, in_specs):
    return pl.pallas_call(
        body,
        out_shape=outs,
        in_specs=in_specs,
        out_specs=tuple(pl.BlockSpec(memory_space=VMEM) for _ in outs),
        scratch_shapes=scratch,
        compiler_params=pltpu.CompilerParams(vmem_limit_bytes=VMEM_LIMIT),
        cost_estimate=pl.CostEstimate(flops=flops, bytes_accessed=bytes_accessed, transcendentals=0),
    )


def in_vmem(n):
    return [pl.BlockSpec(memory_space=VMEM)] * n


def held(value):
    return pltpu.with_memory_space_constraint(value, VMEM)


def block_at(where, job, i):
    half, delta, low = job
    j = lax.rem(where[1 - half] + ORDER[low + i], RING)
    far = lax.rem(where[half] + delta, RING)
    return far * RING + j if half == 0 else j * RING + far


def gather_body(wanted, where, parts, *refs):
    outs, sem = refs[:-1], refs[-1]
    copies = []
    for (jobs, mine), out in zip(wanted, outs):
        core = where[2] if mine else 1 - where[2]
        for q, job in enumerate(jobs):
            for i in range(2):
                source = parts.at[block_at(where, job, i), core, job[0]]
                copies.append(pltpu.make_async_copy(source, out.at[q, i], sem.at[len(copies)]))
    for copy in copies:
        copy.start()
    for copy in copies:
        copy.wait()


def gather(where, parts, wanted):
    rows, cols = parts.shape[3:]
    size = 2 * rows * cols * sum(len(jobs) for jobs, _ in wanted)
    return call(
        functools.partial(gather_body, wanted),
        tuple(VMEM((len(jobs), 2, rows, cols), parts.dtype) for jobs, _ in wanted),
        [pltpu.SemaphoreType.DMA((2 * sum(len(jobs) for jobs, _ in wanted),))],
        size,
        4 * size,
        [pl.BlockSpec(memory_space=pltpu.SMEM), pl.BlockSpec(memory_space=pltpu.HBM)],
    )(where, pltpu.with_memory_space_constraint(parts, pltpu.HBM))


def chunks(rows, step, carry):
    return lax.fori_loop(0, rows // STEP, lambda n, c: step(pl.multiple_of(n * STEP, STEP), c), carry)


def fold(values, join):
    folded = values[0:8]
    for at in range(8, values.shape[0], 8):
        folded = join(folded, values[at : at + 8])
    return folded


def send_blocks(total, outs, peaks, rows, each):
    code = scale_code(jnp.concatenate(peaks, axis=0))
    factor = send_factor(code)
    for q, out in enumerate(outs):
        for i in range(each):
            line = q * each + i
            by = factor[line : line + 1]

            def step(r, _, line=line, by=by, out=out, i=i):
                out[pl.ds(i * rows + r, STEP), :] = encode(total[line, pl.ds(r, STEP), :], by)

            chunks(rows, step, None)
        out[each * rows : each * rows + SIDE, :] = side_rows(
            [code[q * each + i : q * each + i + 1] for i in range(each)]
        )


def pair_body(messages, first, relays, sends, *refs):
    (where, parts, came), refs = refs[:3], refs[3:]
    relayed, refs = refs[:relays], refs[relays:]
    outs, total = refs[: len(messages)], refs[-1]
    rows, cols = came.shape[2:]
    core = where[2]
    for out, wanted in zip(refs[len(messages) : -1], sends):
        for q, job in enumerate(wanted):
            for i in range(2):
                at = block_at(where, job, i)
                for r in range(0, rows, STEP):
                    out[q, i, r : r + STEP, :] = parts[at, 1 - core, job[0], r : r + STEP, :]
    peaks, line = [], 0
    for m, blocks in enumerate(messages):
        by = came_factor(relayed[m].at[2 * rows : 2 * rows + SIDE]) if relayed else None
        for job, q, i in blocks:
            at = (q, i) if first else (block_at(where, job, i), core, job[0])

            def step(r, peak, m=m, q=q, i=i, by=by, at=at, line=line):
                value = parts[(*at, pl.ds(r, STEP))].astype(F32) + came[q, i, pl.ds(r, STEP), :].astype(F32)
                if relayed:
                    value = value + decode(relayed[m][pl.ds(i * rows + r, STEP), :], by[i : i + 1])
                total[line, pl.ds(r, STEP), :] = value
                return jnp.maximum(peak, fold(jnp.abs(value), jnp.maximum))

            peak = chunks(rows, step, jnp.zeros((8, cols), F32))
            peaks.append(jnp.max(peak, axis=0, keepdims=True))
            line += 1
    send_blocks(total, outs, peaks, rows, len(messages[0]))


def pair(where, parts, came, messages, first=False, relayed=(), sends=()):
    rows, cols = came.shape[2:]
    each, n = len(messages[0]), len(messages)
    got = call(
        functools.partial(pair_body, messages, first, len(relayed), sends),
        (VMEM((each * rows + SIDE, cols), I16),) * n
        + tuple(VMEM((len(wanted), 2, rows, cols), came.dtype) for wanted in sends),
        [VMEM((each * n, rows, cols), F32)],
        50 * each * n * rows * cols,
        6 * each * n * rows * cols,
        [pl.BlockSpec(memory_space=pltpu.SMEM), *in_vmem(2 + len(relayed))],
    )(where, parts, held(came), *[held(r) for r in relayed])
    return got[:n], got[n:]


def column_of(row):
    n = row.shape[1]
    return jnp.transpose(jnp.broadcast_to(row, (128, n)))[:, 0:1]


def row_of(column):
    n = column.shape[0]
    return jnp.transpose(jnp.broadcast_to(column, (n, 128)))[0:1, :]


def keep_body(jobs, where, parts, came, *refs):
    got, total = refs[:4], refs[4]
    rows = came.shape[2]
    for half in range(2):
        for i in range(RING):
            ref = got[2 * half + (1 if i < 2 else 0)]
            by = came_factor(ref.at[2 * rows : 2 * rows + SIDE])[i % 2 : i % 2 + 1]
            q = 2 * half + i // 2
            at = (block_at(where, jobs[q], i % 2), where[2], half)

            def step(r, _, ref=ref, by=by, half=half, i=i, q=q, at=at):
                value = parts[(*at, pl.ds(r, STEP))].astype(F32) + came[q, i % 2, pl.ds(r, STEP), :].astype(F32)
                total[half, i, pl.ds(r, STEP), :] = value + decode(ref[pl.ds(i % 2 * rows + r, STEP), :], by)

            chunks(rows, step, None)


def keep(where, parts, came, jobs, got):
    rows, cols = came.shape[2:]
    return call(
        functools.partial(keep_body, jobs),
        (VMEM((2, RING, rows, cols), F32),),
        [],
        200 * rows * cols,
        80 * rows * cols,
        [pl.BlockSpec(memory_space=pltpu.SMEM), *in_vmem(6)],
    )(where, parts, held(came), *[held(g) for g in got])[0]


def old_body(*refs):
    for (codes, row, column, out), levels, beta in (
        ((*refs[:3], refs[6]), 7.0, beta_first),
        ((*refs[3:6], refs[7]), 15.0, beta_second),
    ):
        tall, wide = column_of(row[...]), column[...]
        for r in range(0, out.shape[0], STEP):
            bound = jnp.minimum(tall[r : r + STEP], wide)
            out[r : r + STEP, :] = codes[0, r : r + STEP, :].astype(F32) * (beta / levels) * bound


def old_moments(old):
    _, rows, cols = old[0].shape
    each = VMEM((rows, cols), F32)
    return call(old_body, (each, each), [], 10 * rows * cols, 16 * rows * cols, in_vmem(6))(*old)


def middle_body(half, blocks, sent, acc, first, second, *refs):
    outs, total = refs[:-1], refs[-1]
    rows, cols = acc.shape[2:]
    peaks = []
    for n, (i, ref) in enumerate(zip(blocks, (first, second))):
        by = came_factor(ref.at[rows : rows + SIDE])[0:1]

        def step(r, peak, ref=ref, by=by, i=i, n=n):
            value = acc[half, i, pl.ds(r, STEP), :] + decode(ref[pl.ds(r, STEP), :], by)
            if n >= sent:
                outs[n][pl.ds(r, STEP), :] = value
                return peak
            total[n, pl.ds(r, STEP), :] = value
            return jnp.maximum(peak, fold(jnp.abs(value), jnp.maximum))

        peak = chunks(rows, step, jnp.zeros((8, cols), F32))
        if n < sent:
            peaks.append(jnp.max(peak, axis=0, keepdims=True))
    send_blocks(total, outs[:sent], peaks, rows, 1)


def middle(acc, got, half, blocks, sent):
    rows, cols = acc.shape[2:]
    return call(
        functools.partial(middle_body, half, blocks, sent),
        tuple(VMEM((rows + SIDE, cols), I16) if n < sent else VMEM((rows, cols), F32) for n in range(2)),
        [VMEM((sent, rows, cols), F32)],
        100 * rows * cols,
        16 * rows * cols,
        in_vmem(3),
    )(acc, *[held(g) for g in got])


def last_body(*refs):
    ins, (grad, squares) = refs[:8], refs[8:]
    rows, cols = ins[0].shape
    square = jnp.zeros((8, cols), F32)
    for half in range(2):
        kept, *got = ins[4 * half : 4 * half + 4]
        by = [came_factor(ref.at[rows : rows + SIDE])[0:1] for ref in got]

        def step(r, square, half=half, kept=kept, got=got, by=by):
            value = kept[pl.ds(r, STEP), :]
            for ref, factor in zip(got, by):
                value = value + decode(ref[pl.ds(r, STEP), :], factor)
            grad[pl.ds(half * rows + r, STEP), :] = value
            return square + fold(value * value, jnp.add)

        square = chunks(rows, step, square)
    folded = square[:, 0:128]
    for at in range(128, cols, 128):
        folded = folded + square[:, at : at + 128]
    squares[...] = jnp.broadcast_to(jnp.sum(folded, axis=0, keepdims=True), squares.shape)


def last(halves, devices):
    rows, cols = halves[0][0].shape
    flat = [a for kept, *got in halves for a in (kept, *[held(g) for g in got])]
    return call(
        last_body,
        (VMEM((2 * rows, cols), F32), VMEM((devices, 128), F32)),
        [],
        100 * rows * cols,
        32 * rows * cols,
        in_vmem(8),
    )(*flat)


def reduce_scatter(parts, devices):
    where = jnp.stack([lax.axis_index(a) for a in FSDP]).astype(jnp.int32)
    resident = held(parts)
    axis = ("y", "z")

    def hop(value, name, delta):
        return lax.ppermute(value, name, [(i, (i + delta) % RING) for i in range(RING)])

    def swap(value):
        return lax.ppermute(value, "core", [(0, 1), (1, 0)])

    def stage(half, messages, came, source=resident, first=False, relayed=(), sends=()):
        sent, more = pair(where, source, came, messages, first, relayed, sends)
        got = []
        for value, delta in zip(sent, (1, 3)):
            got.append(hop(value, axis[half], delta))
        return got, more

    def jobs_of(*each):
        return [tuple((half, delta, low) for delta, low in each) for half in range(2)]

    def blocks_of(jobs, base=0, only=(0, 1)):
        return tuple(tuple((job, base + q, i) for i in only) for q, job in enumerate(jobs))

    far, near = jobs_of((2, 0), (2, 2)), jobs_of((1, 2), (3, 0))
    join, mine = jobs_of((1, 0), (3, 2)), jobs_of((0, 0), (0, 2))
    (out,) = gather(where, parts, ((far[0], False),))
    came_far_0 = swap(out)
    out, own_far_0 = gather(where, parts, ((far[1], False), (far[0], True)))
    came_far_1 = swap(out)
    far_0, _ = stage(0, blocks_of(far[0]), came_far_0, own_far_0, True)
    far_1, out = stage(1, blocks_of(far[1]), came_far_1, sends=near)
    came_near = [swap(o) for o in out]
    near_0, (out,) = stage(0, blocks_of(near[0]), came_near[0], sends=(join[0] + join[1],))
    came_join = swap(out)
    near_1, (out,) = stage(1, blocks_of(near[1]), came_near[1], sends=(mine[0] + mine[1],))
    came_mine = swap(out)
    joined = {}
    for only in range(2):
        for half, relayed in enumerate((far_0, far_1)):
            messages = blocks_of(join[half], 2 * half, (only,))
            joined[only, half], _ = stage(half, messages, came_join, relayed=relayed)
    acc = keep(where, resident, came_mine, mine[0] + mine[1], (*near_0, *near_1))
    halves = []
    for half in range(2):
        near_out, far_out = middle(acc, joined[0, half], half, (0, 2), 2)
        back_out, kept = middle(acc, joined[1, half], half, (1, 3), 1)
        got = []
        for out, delta in ((far_out, 2), (near_out, 1), (back_out, 3)):
            got.append(hop(out, axis[1 - half], delta))
        halves.append([kept] + got)
    return last(halves, devices)


def clip_body(limit, squares, grad, first_old, second_old, first_new, second_new, peaks):
    rows, cols = grad.shape
    total = jnp.sum(jnp.sum(squares[...], axis=0, keepdims=True), axis=1, keepdims=True)
    scale = limit / jnp.maximum(jnp.sqrt(total), limit)

    def step(r, peak):
        clipped = grad[pl.ds(r, STEP), :] * scale
        first = first_old[pl.ds(r, STEP), :] + (1.0 - beta_first) * clipped
        second = second_old[pl.ds(r, STEP), :] + (1.0 - beta_second) * clipped * clipped
        first_new[pl.ds(r, STEP), :] = first
        second_new[pl.ds(r, STEP), :] = second
        return (
            jnp.maximum(peak[0], fold(jnp.abs(first), jnp.maximum)),
            jnp.maximum(peak[1], fold(second, jnp.maximum)),
        )

    zero = jnp.zeros((8, cols), F32)
    found = chunks(rows, step, (zero, zero))
    lines = []
    for peak in found:
        peak = jnp.max(peak, axis=0, keepdims=True)
        lines += [peak[:, at : at + 128] for at in range(0, cols, 128)]
    lines = jnp.concatenate(lines, axis=0)
    for at in range(peaks.shape[0]):
        peaks[at] = lines


def clip(squares, grad, first_old, second_old, limit, group):
    rows, cols = grad.shape
    each = VMEM((rows, cols), F32)
    return call(
        functools.partial(clip_body, limit),
        (each, each, VMEM((group, 2 * cols // 128, 128), F32)),
        [],
        12 * rows * cols,
        20 * rows * cols,
        in_vmem(4),
    )(held(squares), grad, first_old, second_old)


def rows_body(first_new, second_new, direction, first_rowmax, second_rowmax, by_first, by_second):
    first, second = first_new[...], second_new[...]
    direction[0] = first / (jnp.sqrt(second) + epsilon)
    for values, least, peak, by in (
        (jnp.abs(first), scale_floor, first_rowmax, by_first),
        (second, 0.0, second_rowmax, by_second),
    ):
        tall = jnp.maximum(jnp.max(values, axis=1, keepdims=True), least)
        by[...] = jnp.broadcast_to(1.0 / tall, by.shape)
        peak[...] = row_of(tall)


def row_outputs(first_new, second_new):
    rows, cols = first_new.shape
    step = min(rows, 128)
    whole = pl.BlockSpec((step, cols), lambda r: (r, 0))
    side, line = pl.BlockSpec((step, 128), lambda r: (r, 0)), pl.BlockSpec((1, step), lambda r: (0, r))
    return pl.pallas_call(
        rows_body,
        grid=(rows // step,),
        out_shape=(
            jax.ShapeDtypeStruct((1, rows, cols), F32),
            jax.ShapeDtypeStruct((1, rows), F32),
            jax.ShapeDtypeStruct((1, rows), F32),
            VMEM((rows, 128), F32),
            VMEM((rows, 128), F32),
        ),
        in_specs=[whole, whole],
        out_specs=(pl.BlockSpec((1, step, cols), lambda r: (0, r, 0)), line, line, side, side),
        compiler_params=pltpu.CompilerParams(vmem_limit_bytes=VMEM_LIMIT),
        cost_estimate=pl.CostEstimate(flops=40 * rows * cols, bytes_accessed=12 * rows * cols, transcendentals=0),
        name="row_outputs",
    )(first_new, second_new)


def scaled_body(peaks, first_new, second_new, by_first, by_second, *refs):
    first_scaled, second_scaled, first_colmax, second_colmax, inverse = refs
    half = peaks.shape[1] // 2

    @pl.when(pl.program_id(0) == 0)
    def _():
        found = jnp.max(peaks[...], axis=0)
        for k, (out, least) in enumerate(((first_colmax, scale_floor), (second_colmax, 0.0))):
            wide = [found[k * half + at : k * half + at + 1] for at in range(half)]
            wide = jnp.maximum(jnp.concatenate(wide, axis=1), least)
            out[...] = wide
            inverse[k : k + 1, :] = 1.0 / wide

    step = first_scaled.shape[1]
    rows = pl.ds(pl.multiple_of(pl.program_id(0) * step, step), step)
    for k, (values, by, out) in enumerate(
        ((first_new, by_first, first_scaled), (second_new, by_second, second_scaled))
    ):
        out[0] = values[rows, :] * jnp.maximum(by[rows, 0:1], inverse[k : k + 1, :])


def scaled_outputs(peaks, first_new, second_new, by_first, by_second):
    rows, cols = first_new.shape
    step = min(rows, 64)
    out, line = pl.BlockSpec((1, step, cols), lambda r: (0, r, 0)), pl.BlockSpec((1, cols), lambda r: (0, 0))
    big, wide = jax.ShapeDtypeStruct((1, rows, cols), F32), jax.ShapeDtypeStruct((1, cols), F32)
    return pl.pallas_call(
        scaled_body,
        grid=(rows // step,),
        out_shape=(big, big, wide, wide),
        in_specs=in_vmem(5),
        out_specs=(out, out, line, line),
        scratch_shapes=[VMEM((8, cols), F32)],
        compiler_params=pltpu.CompilerParams(vmem_limit_bytes=VMEM_LIMIT),
        cost_estimate=pl.CostEstimate(flops=8 * rows * cols, bytes_accessed=16 * rows * cols, transcendentals=0),
        name="scaled_outputs",
    )(held(peaks), first_new, second_new, by_first, by_second)


def exchange(value, axes):
    return lax.all_to_all(value, axes, split_axis=0, concat_axis=0, tiled=True)


def local(
    grad_parts, first_codes, first_rows, first_columns, second_codes, second_rows, second_columns
):
    layer_count, _, row_count, col_count = grad_parts.shape
    entries = layer_count * lax.axis_size("section") * row_count * col_count
    devices, group = lax.axis_size(AXES), lax.axis_size(FSDP)
    parts = grad_parts.reshape(RING * RING, 2, 2, -1, col_count)
    old = (first_codes, first_rows, first_columns, second_codes, second_rows, second_columns)
    gradient, squares = reduce_scatter(parts, devices)
    first_old, second_old = old_moments(old)
    squares = exchange(squares, AXES)
    clip_limit = clip_rms * math.sqrt(entries)
    first_new, second_new, peaks = clip(squares, gradient, first_old, second_old, clip_limit, group)
    peaks = exchange(peaks, FSDP)
    direction, first_rowmax, second_rowmax, by_first, by_second = row_outputs(first_new, second_new)
    first_scaled, second_scaled, first_colmax, second_colmax = scaled_outputs(
        peaks, first_new, second_new, by_first, by_second
    )
    return (
        direction,
        first_scaled,
        second_scaled,
        first_rowmax,
        first_colmax,
        second_rowmax,
        second_colmax,
    )


def solution(mesh):
    torus = Mesh(mesh.devices.reshape(mesh.shape["section"], RING, RING, 2), AXES)
    placed = (
        P("section", FSDP, None, None),
        P("section", FSDP, None),
        P("section", FSDP),
        P("section", None),
        P("section", FSDP, None),
        P("section", FSDP),
        P("section", None),
    )
    return jax.shard_map(
        local,
        mesh=torus,
        in_specs=placed,
        out_specs=(
            P("section", FSDP, None),
            P("section", FSDP, None),
            P("section", FSDP, None),
            P("section", FSDP),
            P("section", None),
            P("section", FSDP),
            P("section", None),
        ),
        check_vma=False,
    )
```

```python
import functools
import math

import jax
import jax.numpy as jnp
from jax import lax
from jax.experimental import pallas as pl
from jax.experimental.pallas import tpu as pltpu
from jax.sharding import Mesh
from jax.sharding import PartitionSpec as P


AXES = ("section", "y", "z", "core")
FSDP = ("y", "z", "core")

beta_first = 0.9
beta_second = 0.999
clip_rms = 3.0
epsilon = 1e-08
scale_floor = 0.001

RING = 4
ORDER = (1, 3, 2, 0)
TOP = 32767.0
LEAST = 1e-18
SIDE = 8
STEP = 64
VMEM_LIMIT = 8 * 1024 * 1024
F32, I16 = jnp.float32, jnp.int16
VMEM = pltpu.VMEM


def scale_code(peak):
    return jnp.ceil(jnp.log2(jnp.maximum(peak, LEAST)) * 256.0)


def send_factor(code):
    return jnp.exp2(code * (-1.0 / 256.0)) * TOP**4


def encode(values, factor):
    root = lax.rsqrt(lax.rsqrt(jnp.abs(values) * factor))
    root = jnp.where(values < 0.0, -root, root)
    return jnp.round(root).astype(jnp.int32).astype(I16)


def came_factor(side):
    code = side[...].astype(jnp.int32).astype(F32)
    return jnp.exp2(code * (1.0 / 256.0)) * TOP**-4


def decode(codes, factor):
    root = codes.astype(jnp.int32).astype(F32)
    square = root * jnp.abs(root)
    return (square * jnp.abs(square)) * factor


def side_rows(codes):
    line = lax.broadcasted_iota(jnp.int32, (SIDE, codes[0].shape[1]), 0)
    rows = codes[-1]
    for at, code in enumerate(codes[:-1]):
        rows = jnp.where(line == at, code, rows)
    return jnp.broadcast_to(rows, line.shape).astype(jnp.int32).astype(I16)


def call(body, outs, scratch, flops, bytes_accessed, in_specs):
    return pl.pallas_call(
        body,
        out_shape=outs,
        in_specs=in_specs,
        out_specs=tuple(pl.BlockSpec(memory_space=VMEM) for _ in outs),
        scratch_shapes=scratch,
        compiler_params=pltpu.CompilerParams(vmem_limit_bytes=VMEM_LIMIT),
        cost_estimate=pl.CostEstimate(flops=flops, bytes_accessed=bytes_accessed, transcendentals=0),
    )


def in_vmem(n):
    return [pl.BlockSpec(memory_space=VMEM)] * n


def held(value):
    return pltpu.with_memory_space_constraint(value, VMEM)


def position():
    return [lax.axis_index(a) for a in FSDP]


def block_at(where, job, i):
    half, delta, low = job
    j = lax.rem(where[1 - half] + ORDER[low + i], RING)
    far = lax.rem(where[half] + delta, RING)
    return far * RING + j if half == 0 else j * RING + far


def gather_body(wanted, parts, *refs):
    outs, sem = refs[:-1], refs[-1]
    where = position()
    copies = []
    for (jobs, mine), out in zip(wanted, outs):
        core = where[2] if mine else 1 - where[2]
        for q, job in enumerate(jobs):
            for i in range(2):
                source = parts.at[block_at(where, job, i), core, job[0]]
                copies.append(pltpu.make_async_copy(source, out.at[q, i], sem.at[len(copies)]))
    for copy in copies:
        copy.start()
    for copy in copies:
        copy.wait()


def gather(parts, wanted):
    rows, cols = parts.shape[3:]
    size = 2 * rows * cols * sum(len(jobs) for jobs, _ in wanted)
    return call(
        functools.partial(gather_body, wanted),
        tuple(VMEM((len(jobs), 2, rows, cols), parts.dtype) for jobs, _ in wanted),
        [pltpu.SemaphoreType.DMA((2 * sum(len(jobs) for jobs, _ in wanted),))],
        size,
        4 * size,
        [pl.BlockSpec(memory_space=pltpu.HBM)],
    )(pltpu.with_memory_space_constraint(parts, pltpu.HBM))


def chunks(rows, step, carry):
    return lax.fori_loop(0, rows // STEP, lambda n, c: step(pl.multiple_of(n * STEP, STEP), c), carry)


def fold(values, join):
    folded = values[0:8]
    for at in range(8, values.shape[0], 8):
        folded = join(folded, values[at : at + 8])
    return folded


def send_blocks(total, outs, peaks, rows, each):
    code = scale_code(jnp.concatenate(peaks, axis=0))
    factor = send_factor(code)
    for q, out in enumerate(outs):
        for i in range(each):
            line = q * each + i
            by = factor[line : line + 1]

            def step(r, _, line=line, by=by, out=out, i=i):
                out[pl.ds(i * rows + r, STEP), :] = encode(total[line, pl.ds(r, STEP), :], by)

            chunks(rows, step, None)
        out[each * rows : each * rows + SIDE, :] = side_rows(
            [code[q * each + i : q * each + i + 1] for i in range(each)]
        )


def pair_body(messages, first, relays, sends, *refs):
    (parts, came), refs = refs[:2], refs[2:]
    where = position()
    relayed, refs = refs[:relays], refs[relays:]
    outs, total = refs[: len(messages)], refs[-1]
    rows, cols = came.shape[2:]
    core = where[2]
    for out, wanted in zip(refs[len(messages) : -1], sends):
        for q, job in enumerate(wanted):
            for i in range(2):
                at = block_at(where, job, i)
                for r in range(0, rows, STEP):
                    out[q, i, r : r + STEP, :] = parts[at, 1 - core, job[0], r : r + STEP, :]
    peaks, line = [], 0
    for m, blocks in enumerate(messages):
        by = came_factor(relayed[m].at[2 * rows : 2 * rows + SIDE]) if relayed else None
        for job, q, i in blocks:
            at = (q, i) if first else (block_at(where, job, i), core, job[0])

            def step(r, peak, m=m, q=q, i=i, by=by, at=at, line=line):
                value = parts[(*at, pl.ds(r, STEP))].astype(F32) + came[q, i, pl.ds(r, STEP), :].astype(F32)
                if relayed:
                    value = value + decode(relayed[m][pl.ds(i * rows + r, STEP), :], by[i : i + 1])
                total[line, pl.ds(r, STEP), :] = value
                return jnp.maximum(peak, fold(jnp.abs(value), jnp.maximum))

            peak = chunks(rows, step, jnp.zeros((8, cols), F32))
            peaks.append(jnp.max(peak, axis=0, keepdims=True))
            line += 1
    send_blocks(total, outs, peaks, rows, len(messages[0]))


def pair(parts, came, messages, first=False, relayed=(), sends=()):
    rows, cols = came.shape[2:]
    each, n = len(messages[0]), len(messages)
    got = call(
        functools.partial(pair_body, messages, first, len(relayed), sends),
        (VMEM((each * rows + SIDE, cols), I16),) * n
        + tuple(VMEM((len(wanted), 2, rows, cols), came.dtype) for wanted in sends),
        [VMEM((each * n, rows, cols), F32)],
        50 * each * n * rows * cols,
        6 * each * n * rows * cols,
        in_vmem(2 + len(relayed)),
    )(parts, held(came), *[held(r) for r in relayed])
    return got[:n], got[n:]


def column_of(row):
    n = row.shape[1]
    return jnp.transpose(jnp.broadcast_to(row, (128, n)))[:, 0:1]


def row_of(column):
    n = column.shape[0]
    return jnp.transpose(jnp.broadcast_to(column, (n, 128)))[0:1, :]


def keep_body(jobs, parts, came, *refs):
    got, total = refs[:4], refs[4]
    where = position()
    rows = came.shape[2]
    for half in range(2):
        for i in range(RING):
            ref = got[2 * half + (1 if i < 2 else 0)]
            by = came_factor(ref.at[2 * rows : 2 * rows + SIDE])[i % 2 : i % 2 + 1]
            q = 2 * half + i // 2
            at = (block_at(where, jobs[q], i % 2), where[2], half)

            def step(r, _, ref=ref, by=by, half=half, i=i, q=q, at=at):
                value = parts[(*at, pl.ds(r, STEP))].astype(F32) + came[q, i % 2, pl.ds(r, STEP), :].astype(F32)
                total[half, i, pl.ds(r, STEP), :] = value + decode(ref[pl.ds(i % 2 * rows + r, STEP), :], by)

            chunks(rows, step, None)


def keep(parts, came, jobs, got):
    rows, cols = came.shape[2:]
    return call(
        functools.partial(keep_body, jobs),
        (VMEM((2, RING, rows, cols), F32),),
        [],
        200 * rows * cols,
        80 * rows * cols,
        in_vmem(6),
    )(parts, held(came), *[held(g) for g in got])[0]


def old_body(*refs):
    for (codes, row, column, out), levels, beta in (
        ((*refs[:3], refs[6]), 7.0, beta_first),
        ((*refs[3:6], refs[7]), 15.0, beta_second),
    ):
        tall, wide = column_of(row[...]), column[...]
        for r in range(0, out.shape[0], STEP):
            bound = jnp.minimum(tall[r : r + STEP], wide)
            out[r : r + STEP, :] = codes[0, r : r + STEP, :].astype(F32) * (beta / levels) * bound


def old_moments(old):
    _, rows, cols = old[0].shape
    each = VMEM((rows, cols), F32)
    return call(old_body, (each, each), [], 10 * rows * cols, 16 * rows * cols, in_vmem(6))(*old)


def middle_body(half, blocks, sent, acc, first, second, *refs):
    outs, total = refs[:-1], refs[-1]
    rows, cols = acc.shape[2:]
    peaks = []
    for n, (i, ref) in enumerate(zip(blocks, (first, second))):
        by = came_factor(ref.at[rows : rows + SIDE])[0:1]

        def step(r, peak, ref=ref, by=by, i=i, n=n):
            value = acc[half, i, pl.ds(r, STEP), :] + decode(ref[pl.ds(r, STEP), :], by)
            if n >= sent:
                outs[n][pl.ds(r, STEP), :] = value
                return peak
            total[n, pl.ds(r, STEP), :] = value
            return jnp.maximum(peak, fold(jnp.abs(value), jnp.maximum))

        peak = chunks(rows, step, jnp.zeros((8, cols), F32))
        if n < sent:
            peaks.append(jnp.max(peak, axis=0, keepdims=True))
    send_blocks(total, outs[:sent], peaks, rows, 1)


def middle(acc, got, half, blocks, sent):
    rows, cols = acc.shape[2:]
    return call(
        functools.partial(middle_body, half, blocks, sent),
        tuple(VMEM((rows + SIDE, cols), I16) if n < sent else VMEM((rows, cols), F32) for n in range(2)),
        [VMEM((sent, rows, cols), F32)],
        100 * rows * cols,
        16 * rows * cols,
        in_vmem(3),
    )(acc, *[held(g) for g in got])


def last_body(*refs):
    ins, (grad, squares) = refs[:8], refs[8:]
    rows, cols = ins[0].shape
    square = jnp.zeros((8, cols), F32)
    for half in range(2):
        kept, *got = ins[4 * half : 4 * half + 4]
        by = [came_factor(ref.at[rows : rows + SIDE])[0:1] for ref in got]

        def step(r, square, half=half, kept=kept, got=got, by=by):
            value = kept[pl.ds(r, STEP), :]
            for ref, factor in zip(got, by):
                value = value + decode(ref[pl.ds(r, STEP), :], factor)
            grad[pl.ds(half * rows + r, STEP), :] = value
            return square + fold(value * value, jnp.add)

        square = chunks(rows, step, square)
    folded = square[:, 0:128]
    for at in range(128, cols, 128):
        folded = folded + square[:, at : at + 128]
    squares[...] = jnp.broadcast_to(jnp.sum(folded, axis=0, keepdims=True), squares.shape)


def last(halves, devices):
    rows, cols = halves[0][0].shape
    flat = [a for kept, *got in halves for a in (kept, *[held(g) for g in got])]
    return call(
        last_body,
        (VMEM((2 * rows, cols), F32), VMEM((devices, 128), F32)),
        [],
        100 * rows * cols,
        32 * rows * cols,
        in_vmem(8),
    )(*flat)


def reduce_scatter(parts, devices):
    resident = held(parts)
    axis = ("y", "z")

    def hop(value, name, delta):
        return lax.ppermute(value, name, [(i, (i + delta) % RING) for i in range(RING)])

    def swap(value):
        return lax.ppermute(value, "core", [(0, 1), (1, 0)])

    def stage(half, messages, came, source=resident, first=False, relayed=(), sends=()):
        sent, more = pair(source, came, messages, first, relayed, sends)
        got = []
        for value, delta in zip(sent, (1, 3)):
            got.append(hop(value, axis[half], delta))
        return got, more

    def jobs_of(*each):
        return [tuple((half, delta, low) for delta, low in each) for half in range(2)]

    def blocks_of(jobs, base=0, only=(0, 1)):
        return tuple(tuple((job, base + q, i) for i in only) for q, job in enumerate(jobs))

    far, near = jobs_of((2, 0), (2, 2)), jobs_of((1, 2), (3, 0))
    join, mine = jobs_of((1, 0), (3, 2)), jobs_of((0, 0), (0, 2))
    (out,) = gather(parts, ((far[0], False),))
    came_far_0 = swap(out)
    out, own_far_0 = gather(parts, ((far[1], False), (far[0], True)))
    came_far_1 = swap(out)
    far_0, _ = stage(0, blocks_of(far[0]), came_far_0, own_far_0, True)
    far_1, out = stage(1, blocks_of(far[1]), came_far_1, sends=near)
    came_near = [swap(o) for o in out]
    near_0, (out,) = stage(0, blocks_of(near[0]), came_near[0], sends=(join[0] + join[1],))
    came_join = swap(out)
    near_1, (out,) = stage(1, blocks_of(near[1]), came_near[1], sends=(mine[0] + mine[1],))
    came_mine = swap(out)
    joined = {}
    for only in range(2):
        for half, relayed in enumerate((far_0, far_1)):
            messages = blocks_of(join[half], 2 * half, (only,))
            joined[only, half], _ = stage(half, messages, came_join, relayed=relayed)
    acc = keep(resident, came_mine, mine[0] + mine[1], (*near_0, *near_1))
    halves = []
    for half in range(2):
        near_out, far_out = middle(acc, joined[0, half], half, (0, 2), 2)
        back_out, kept = middle(acc, joined[1, half], half, (1, 3), 1)
        got = []
        for out, delta in ((far_out, 2), (near_out, 1), (back_out, 3)):
            got.append(hop(out, axis[1 - half], delta))
        halves.append([kept] + got)
    return last(halves, devices)


def clip_body(limit, squares, grad, first_old, second_old, first_new, second_new, peaks):
    rows, cols = grad.shape
    total = jnp.sum(jnp.sum(squares[...], axis=0, keepdims=True), axis=1, keepdims=True)
    scale = limit / jnp.maximum(jnp.sqrt(total), limit)

    def step(r, peak):
        clipped = grad[pl.ds(r, STEP), :] * scale
        first = first_old[pl.ds(r, STEP), :] + (1.0 - beta_first) * clipped
        second = second_old[pl.ds(r, STEP), :] + (1.0 - beta_second) * clipped * clipped
        first_new[pl.ds(r, STEP), :] = first
        second_new[pl.ds(r, STEP), :] = second
        return (
            jnp.maximum(peak[0], fold(jnp.abs(first), jnp.maximum)),
            jnp.maximum(peak[1], fold(second, jnp.maximum)),
        )

    zero = jnp.zeros((8, cols), F32)
    found = chunks(rows, step, (zero, zero))
    lines = []
    for peak in found:
        peak = jnp.max(peak, axis=0, keepdims=True)
        lines += [peak[:, at : at + 128] for at in range(0, cols, 128)]
    lines = jnp.concatenate(lines, axis=0)
    for at in range(peaks.shape[0]):
        peaks[at] = lines


def clip(squares, grad, first_old, second_old, limit, group):
    rows, cols = grad.shape
    each = VMEM((rows, cols), F32)
    return call(
        functools.partial(clip_body, limit),
        (each, each, VMEM((group, 2 * cols // 128, 128), F32)),
        [],
        12 * rows * cols,
        20 * rows * cols,
        in_vmem(4),
    )(held(squares), grad, first_old, second_old)


def rows_body(first_new, second_new, direction, first_rowmax, second_rowmax, by_first, by_second):
    first, second = first_new[...], second_new[...]
    direction[0] = first / (jnp.sqrt(second) + epsilon)
    for values, least, peak, by in (
        (jnp.abs(first), scale_floor, first_rowmax, by_first),
        (second, 0.0, second_rowmax, by_second),
    ):
        tall = jnp.maximum(jnp.max(values, axis=1, keepdims=True), least)
        by[...] = jnp.broadcast_to(1.0 / tall, by.shape)
        peak[...] = row_of(tall)


def row_outputs(first_new, second_new):
    rows, cols = first_new.shape
    step = min(rows, 128)
    whole = pl.BlockSpec((step, cols), lambda r: (r, 0))
    side, line = pl.BlockSpec((step, 128), lambda r: (r, 0)), pl.BlockSpec((1, step), lambda r: (0, r))
    return pl.pallas_call(
        rows_body,
        grid=(rows // step,),
        out_shape=(
            jax.ShapeDtypeStruct((1, rows, cols), F32),
            jax.ShapeDtypeStruct((1, rows), F32),
            jax.ShapeDtypeStruct((1, rows), F32),
            VMEM((rows, 128), F32),
            VMEM((rows, 128), F32),
        ),
        in_specs=[whole, whole],
        out_specs=(pl.BlockSpec((1, step, cols), lambda r: (0, r, 0)), line, line, side, side),
        compiler_params=pltpu.CompilerParams(vmem_limit_bytes=VMEM_LIMIT),
        cost_estimate=pl.CostEstimate(flops=40 * rows * cols, bytes_accessed=12 * rows * cols, transcendentals=0),
        name="row_outputs",
    )(first_new, second_new)


def scaled_body(peaks, first_new, second_new, by_first, by_second, *refs):
    first_scaled, second_scaled, first_colmax, second_colmax, inverse = refs
    half = peaks.shape[1] // 2

    @pl.when(pl.program_id(0) == 0)
    def _():
        found = jnp.max(peaks[...], axis=0)
        for k, (out, least) in enumerate(((first_colmax, scale_floor), (second_colmax, 0.0))):
            wide = [found[k * half + at : k * half + at + 1] for at in range(half)]
            wide = jnp.maximum(jnp.concatenate(wide, axis=1), least)
            out[...] = wide
            inverse[k : k + 1, :] = 1.0 / wide

    step = first_scaled.shape[1]
    rows = pl.ds(pl.multiple_of(pl.program_id(0) * step, step), step)
    for k, (values, by, out) in enumerate(
        ((first_new, by_first, first_scaled), (second_new, by_second, second_scaled))
    ):
        out[0] = values[rows, :] * jnp.maximum(by[rows, 0:1], inverse[k : k + 1, :])


def scaled_outputs(peaks, first_new, second_new, by_first, by_second):
    rows, cols = first_new.shape
    step = min(rows, 64)
    out, line = pl.BlockSpec((1, step, cols), lambda r: (0, r, 0)), pl.BlockSpec((1, cols), lambda r: (0, 0))
    big, wide = jax.ShapeDtypeStruct((1, rows, cols), F32), jax.ShapeDtypeStruct((1, cols), F32)
    return pl.pallas_call(
        scaled_body,
        grid=(rows // step,),
        out_shape=(big, big, wide, wide),
        in_specs=in_vmem(5),
        out_specs=(out, out, line, line),
        scratch_shapes=[VMEM((8, cols), F32)],
        compiler_params=pltpu.CompilerParams(vmem_limit_bytes=VMEM_LIMIT),
        cost_estimate=pl.CostEstimate(flops=8 * rows * cols, bytes_accessed=16 * rows * cols, transcendentals=0),
        name="scaled_outputs",
    )(held(peaks), first_new, second_new, by_first, by_second)


def exchange(value, axes):
    return lax.all_to_all(value, axes, split_axis=0, concat_axis=0, tiled=True)


def local(
    grad_parts, first_codes, first_rows, first_columns, second_codes, second_rows, second_columns
):
    layer_count, _, row_count, col_count = grad_parts.shape
    entries = layer_count * lax.axis_size("section") * row_count * col_count
    devices, group = lax.axis_size(AXES), lax.axis_size(FSDP)
    parts = grad_parts.reshape(RING * RING, 2, 2, -1, col_count)
    old = (first_codes, first_rows, first_columns, second_codes, second_rows, second_columns)
    gradient, squares = reduce_scatter(parts, devices)
    first_old, second_old = old_moments(old)
    squares = exchange(squares, AXES)
    clip_limit = clip_rms * math.sqrt(entries)
    first_new, second_new, peaks = clip(squares, gradient, first_old, second_old, clip_limit, group)
    peaks = exchange(peaks, FSDP)
    direction, first_rowmax, second_rowmax, by_first, by_second = row_outputs(first_new, second_new)
    first_scaled, second_scaled, first_colmax, second_colmax = scaled_outputs(
        peaks, first_new, second_new, by_first, by_second
    )
    return (
        direction,
        first_scaled,
        second_scaled,
        first_rowmax,
        first_colmax,
        second_rowmax,
        second_colmax,
    )


def solution(mesh):
    torus = Mesh(mesh.devices.reshape(mesh.shape["section"], RING, RING, 2), AXES)
    placed = (
        P("section", FSDP, None, None),
        P("section", FSDP, None),
        P("section", FSDP),
        P("section", None),
        P("section", FSDP, None),
        P("section", FSDP),
        P("section", None),
    )
    return jax.shard_map(
        local,
        mesh=torus,
        in_specs=placed,
        out_specs=(
            P("section", FSDP, None),
            P("section", FSDP, None),
            P("section", FSDP, None),
            P("section", FSDP),
            P("section", None),
            P("section", FSDP),
            P("section", None),
        ),
        check_vma=False,
    )
```

```python
import functools
import math

import jax
import jax.numpy as jnp
from jax import lax
from jax.experimental import pallas as pl
from jax.experimental.pallas import tpu as pltpu
from jax.sharding import Mesh
from jax.sharding import PartitionSpec as P


AXES = ("section", "y", "z", "core")
FSDP = ("y", "z", "core")

beta_first = 0.9
beta_second = 0.999
clip_rms = 3.0
epsilon = 1e-08
scale_floor = 0.001

RING = 4
ORDER = (1, 3, 2, 0)
TOP = 32767.0
LEAST = 1e-18
SIDE = 8
STEP = 64
VMEM_LIMIT = 8 * 1024 * 1024
F32, I16 = jnp.float32, jnp.int16
VMEM = pltpu.VMEM


def scale_code(peak):
    return jnp.ceil(jnp.log2(jnp.maximum(peak, LEAST)) * 256.0)


def send_factor(code):
    return jnp.exp2(code * (-1.0 / 256.0)) * TOP**4


def encode(values, factor):
    root = lax.rsqrt(lax.rsqrt(jnp.abs(values) * factor))
    root = jnp.where(values < 0.0, -root, root)
    return jnp.round(root).astype(jnp.int32).astype(I16)


def came_factor(side):
    code = side[...].astype(jnp.int32).astype(F32)
    return jnp.exp2(code * (1.0 / 256.0)) * TOP**-4


def decode(codes, factor):
    root = codes.astype(jnp.int32).astype(F32)
    square = root * jnp.abs(root)
    return (square * jnp.abs(square)) * factor


def side_rows(codes):
    line = lax.broadcasted_iota(jnp.int32, (SIDE, codes[0].shape[1]), 0)
    rows = codes[-1]
    for at, code in enumerate(codes[:-1]):
        rows = jnp.where(line == at, code, rows)
    return jnp.broadcast_to(rows, line.shape).astype(jnp.int32).astype(I16)


def call(body, outs, scratch, flops, bytes_accessed, in_specs):
    return pl.pallas_call(
        body,
        out_shape=outs,
        in_specs=in_specs,
        out_specs=tuple(pl.BlockSpec(memory_space=VMEM) for _ in outs),
        scratch_shapes=scratch,
        compiler_params=pltpu.CompilerParams(vmem_limit_bytes=VMEM_LIMIT),
        cost_estimate=pl.CostEstimate(flops=flops, bytes_accessed=bytes_accessed, transcendentals=0),
    )


def in_vmem(n):
    return [pl.BlockSpec(memory_space=VMEM)] * n


def held(value):
    return pltpu.with_memory_space_constraint(value, VMEM)


def position():
    return [lax.axis_index(a) for a in FSDP]


def block_at(where, job, i):
    half, delta, low = job
    j = lax.rem(where[1 - half] + ORDER[low + i], RING)
    far = lax.rem(where[half] + delta, RING)
    return far * RING + j if half == 0 else j * RING + far


def gather_body(wanted, parts, *refs):
    outs, sem = refs[:-1], refs[-1]
    where = position()
    copies = []
    for (jobs, mine), out in zip(wanted, outs):
        core = where[2] if mine else 1 - where[2]
        for q, job in enumerate(jobs):
            for i in range(2):
                source = parts.at[block_at(where, job, i), core, job[0]]
                copies.append(pltpu.make_async_copy(source, out.at[q, i], sem.at[len(copies)]))
    for copy in copies:
        copy.start()
    for copy in copies:
        copy.wait()


def gather(parts, wanted):
    rows, cols = parts.shape[3:]
    size = 2 * rows * cols * sum(len(jobs) for jobs, _ in wanted)
    return call(
        functools.partial(gather_body, wanted),
        tuple(VMEM((len(jobs), 2, rows, cols), parts.dtype) for jobs, _ in wanted),
        [pltpu.SemaphoreType.DMA((2 * sum(len(jobs) for jobs, _ in wanted),))],
        size,
        4 * size,
        [pl.BlockSpec(memory_space=pltpu.HBM)],
    )(pltpu.with_memory_space_constraint(parts, pltpu.HBM))


def chunks(rows, step, carry):
    return lax.fori_loop(0, rows // STEP, lambda n, c: step(pl.multiple_of(n * STEP, STEP), c), carry)


def fold(values, join):
    folded = values[0:8]
    for at in range(8, values.shape[0], 8):
        folded = join(folded, values[at : at + 8])
    return folded


def send_blocks(total, outs, peaks, rows, each):
    code = scale_code(jnp.concatenate(peaks, axis=0))
    factor = send_factor(code)
    for q, out in enumerate(outs):
        for i in range(each):
            line = q * each + i
            by = factor[line : line + 1]

            def step(r, _, line=line, by=by, out=out, i=i):
                out[pl.ds(i * rows + r, STEP), :] = encode(total[line, pl.ds(r, STEP), :], by)

            chunks(rows, step, None)
        out[each * rows : each * rows + SIDE, :] = side_rows(
            [code[q * each + i : q * each + i + 1] for i in range(each)]
        )


def pair_body(messages, first, relays, sends, *refs):
    (parts, came), refs = refs[:2], refs[2:]
    where = position()
    relayed, refs = refs[:relays], refs[relays:]
    outs, total = refs[: len(messages)], refs[-1]
    rows, cols = came.shape[2:]
    core = where[2]
    for out, wanted in zip(refs[len(messages) : -1], sends):
        for q, job in enumerate(wanted):
            for i in range(2):
                at = block_at(where, job, i)
                for r in range(0, rows, STEP):
                    out[q, i, r : r + STEP, :] = parts[at, 1 - core, job[0], r : r + STEP, :]
    peaks, line = [], 0
    for m, blocks in enumerate(messages):
        by = came_factor(relayed[m].at[2 * rows : 2 * rows + SIDE]) if relayed else None
        for job, q, i in blocks:
            at = (q, i) if first else (block_at(where, job, i), core, job[0])

            def step(r, peak, m=m, q=q, i=i, by=by, at=at, line=line):
                value = parts[(*at, pl.ds(r, STEP))].astype(F32) + came[q, i, pl.ds(r, STEP), :].astype(F32)
                if relayed:
                    value = value + decode(relayed[m][pl.ds(i * rows + r, STEP), :], by[i : i + 1])
                total[line, pl.ds(r, STEP), :] = value
                return jnp.maximum(peak, fold(jnp.abs(value), jnp.maximum))

            peak = chunks(rows, step, jnp.zeros((8, cols), F32))
            peaks.append(jnp.max(peak, axis=0, keepdims=True))
            line += 1
    send_blocks(total, outs, peaks, rows, len(messages[0]))


def pair(parts, came, messages, first=False, relayed=(), sends=()):
    rows, cols = came.shape[2:]
    each, n = len(messages[0]), len(messages)
    got = call(
        functools.partial(pair_body, messages, first, len(relayed), sends),
        (VMEM((each * rows + SIDE, cols), I16),) * n
        + tuple(VMEM((len(wanted), 2, rows, cols), came.dtype) for wanted in sends),
        [VMEM((each * n, rows, cols), F32)],
        50 * each * n * rows * cols,
        6 * each * n * rows * cols,
        in_vmem(2 + len(relayed)),
    )(parts, held(came), *[held(r) for r in relayed])
    return got[:n], got[n:]


def column_of(row):
    n = row.shape[1]
    return jnp.transpose(jnp.broadcast_to(row, (128, n)))[:, 0:1]


def row_of(column):
    n = column.shape[0]
    return jnp.transpose(jnp.broadcast_to(column, (n, 128)))[0:1, :]


def keep_body(jobs, parts, came, *refs):
    got, total = refs[:4], refs[4]
    where = position()
    rows = came.shape[2]
    for half in range(2):
        for i in range(RING):
            ref = got[2 * half + (1 if i < 2 else 0)]
            by = came_factor(ref.at[2 * rows : 2 * rows + SIDE])[i % 2 : i % 2 + 1]
            q = 2 * half + i // 2
            at = (block_at(where, jobs[q], i % 2), where[2], half)

            def step(r, _, ref=ref, by=by, half=half, i=i, q=q, at=at):
                value = parts[(*at, pl.ds(r, STEP))].astype(F32) + came[q, i % 2, pl.ds(r, STEP), :].astype(F32)
                total[half, i, pl.ds(r, STEP), :] = value + decode(ref[pl.ds(i % 2 * rows + r, STEP), :], by)

            chunks(rows, step, None)


def keep(parts, came, jobs, got):
    rows, cols = came.shape[2:]
    return call(
        functools.partial(keep_body, jobs),
        (VMEM((2, RING, rows, cols), F32),),
        [],
        200 * rows * cols,
        80 * rows * cols,
        in_vmem(6),
    )(parts, held(came), *[held(g) for g in got])[0]


def old_body(*refs):
    for (codes, row, column, out), levels, beta in (
        ((*refs[:3], refs[6]), 7.0, beta_first),
        ((*refs[3:6], refs[7]), 15.0, beta_second),
    ):
        tall, wide = column_of(row[...]), column[...]
        for r in range(0, out.shape[0], STEP):
            bound = jnp.minimum(tall[r : r + STEP], wide)
            out[r : r + STEP, :] = codes[0, r : r + STEP, :].astype(F32) * (beta / levels) * bound


def old_moments(old):
    _, rows, cols = old[0].shape
    each = VMEM((rows, cols), F32)
    return call(old_body, (each, each), [], 10 * rows * cols, 16 * rows * cols, in_vmem(6))(*old)


def middle_body(half, blocks, sent, acc, first, second, *refs):
    outs, total = refs[:-1], refs[-1]
    rows, cols = acc.shape[2:]
    peaks = []
    for n, (i, ref) in enumerate(zip(blocks, (first, second))):
        by = came_factor(ref.at[rows : rows + SIDE])[0:1]

        def step(r, peak, ref=ref, by=by, i=i, n=n):
            value = acc[half, i, pl.ds(r, STEP), :] + decode(ref[pl.ds(r, STEP), :], by)
            if n >= sent:
                outs[n][pl.ds(r, STEP), :] = value
                return peak
            total[n, pl.ds(r, STEP), :] = value
            return jnp.maximum(peak, fold(jnp.abs(value), jnp.maximum))

        peak = chunks(rows, step, jnp.zeros((8, cols), F32))
        if n < sent:
            peaks.append(jnp.max(peak, axis=0, keepdims=True))
    send_blocks(total, outs[:sent], peaks, rows, 1)


def middle(acc, got, half, blocks, sent):
    rows, cols = acc.shape[2:]
    return call(
        functools.partial(middle_body, half, blocks, sent),
        tuple(VMEM((rows + SIDE, cols), I16) if n < sent else VMEM((rows, cols), F32) for n in range(2)),
        [VMEM((sent, rows, cols), F32)],
        100 * rows * cols,
        16 * rows * cols,
        in_vmem(3),
    )(acc, *[held(g) for g in got])


def early_body(*refs):
    for half in range(2):
        (kept, far), out = refs[2 * half : 2 * half + 2], refs[4 + half]
        rows = kept.shape[0]
        by = came_factor(far.at[rows : rows + SIDE])[0:1]

        def step(r, _, kept=kept, far=far, out=out, by=by):
            out[pl.ds(r, STEP), :] = kept[pl.ds(r, STEP), :] + decode(far[pl.ds(r, STEP), :], by)

        chunks(rows, step, None)


def early(halves):
    rows, cols = halves[0][0].shape
    flat = [a for kept, far, *_ in halves for a in (kept, held(far))]
    return call(early_body, (VMEM((rows, cols), F32),) * 2, [], 40 * rows * cols, 20 * rows * cols, in_vmem(4))(*flat)


def last_body(*refs):
    ins, (grad, squares) = refs[:6], refs[6:]
    rows, cols = ins[0].shape
    square = jnp.zeros((8, cols), F32)
    for half in range(2):
        kept, *got = ins[3 * half : 3 * half + 3]
        by = [came_factor(ref.at[rows : rows + SIDE])[0:1] for ref in got]

        def step(r, square, half=half, kept=kept, got=got, by=by):
            value = kept[pl.ds(r, STEP), :]
            for ref, factor in zip(got, by):
                value = value + decode(ref[pl.ds(r, STEP), :], factor)
            grad[pl.ds(half * rows + r, STEP), :] = value
            return square + fold(value * value, jnp.add)

        square = chunks(rows, step, square)
    folded = square[:, 0:128]
    for at in range(128, cols, 128):
        folded = folded + square[:, at : at + 128]
    squares[...] = jnp.broadcast_to(jnp.sum(folded, axis=0, keepdims=True), squares.shape)


def last(halves, devices):
    rows, cols = halves[0][0].shape
    flat = [a for kept, *got in halves for a in (kept, *[held(g) for g in got])]
    return call(
        last_body,
        (VMEM((2 * rows, cols), F32), VMEM((devices, 128), F32)),
        [],
        80 * rows * cols,
        24 * rows * cols,
        in_vmem(6),
    )(*flat)


def reduce_scatter(parts, devices):
    resident = held(parts)
    axis = ("y", "z")

    def hop(value, name, delta):
        return lax.ppermute(value, name, [(i, (i + delta) % RING) for i in range(RING)])

    def swap(value):
        return lax.ppermute(value, "core", [(0, 1), (1, 0)])

    def stage(half, messages, came, source=resident, first=False, relayed=(), sends=()):
        sent, more = pair(source, came, messages, first, relayed, sends)
        got = []
        for value, delta in zip(sent, (1, 3)):
            got.append(hop(value, axis[half], delta))
        return got, more

    def jobs_of(*each):
        return [tuple((half, delta, low) for delta, low in each) for half in range(2)]

    def blocks_of(jobs, base=0, only=(0, 1)):
        return tuple(tuple((job, base + q, i) for i in only) for q, job in enumerate(jobs))

    far, near = jobs_of((2, 0), (2, 2)), jobs_of((1, 2), (3, 0))
    join, mine = jobs_of((1, 0), (3, 2)), jobs_of((0, 0), (0, 2))
    (out,) = gather(parts, ((far[0], False),))
    came_far_0 = swap(out)
    out, own_far_0 = gather(parts, ((far[1], False), (far[0], True)))
    came_far_1 = swap(out)
    far_0, _ = stage(0, blocks_of(far[0]), came_far_0, own_far_0, True)
    far_1, out = stage(1, blocks_of(far[1]), came_far_1, sends=near)
    came_near = [swap(o) for o in out]
    near_0, (out,) = stage(0, blocks_of(near[0]), came_near[0], sends=(join[0] + join[1],))
    came_join = swap(out)
    near_1, (out,) = stage(1, blocks_of(near[1]), came_near[1], sends=(mine[0] + mine[1],))
    came_mine = swap(out)
    joined = {}
    for only in range(2):
        for half, relayed in enumerate((far_0, far_1)):
            messages = blocks_of(join[half], 2 * half, (only,))
            joined[only, half], _ = stage(half, messages, came_join, relayed=relayed)
    acc = keep(resident, came_mine, mine[0] + mine[1], (*near_0, *near_1))
    halves = []
    for half in range(2):
        near_out, far_out = middle(acc, joined[0, half], half, (0, 2), 2)
        back_out, kept = middle(acc, joined[1, half], half, (1, 3), 1)
        got = []
        for out, delta in ((far_out, 2), (near_out, 1), (back_out, 3)):
            got.append(hop(out, axis[1 - half], delta))
        halves.append([kept] + got)
    sums = early(halves)
    return last([[total, *got[2:]] for total, got in zip(sums, halves)], devices)


def clip_body(limit, squares, grad, first_old, second_old, first_new, second_new, peaks):
    rows, cols = grad.shape
    total = jnp.sum(jnp.sum(squares[...], axis=0, keepdims=True), axis=1, keepdims=True)
    scale = limit / jnp.maximum(jnp.sqrt(total), limit)

    def step(r, peak):
        clipped = grad[pl.ds(r, STEP), :] * scale
        first = first_old[pl.ds(r, STEP), :] + (1.0 - beta_first) * clipped
        second = second_old[pl.ds(r, STEP), :] + (1.0 - beta_second) * clipped * clipped
        first_new[pl.ds(r, STEP), :] = first
        second_new[pl.ds(r, STEP), :] = second
        return (
            jnp.maximum(peak[0], fold(jnp.abs(first), jnp.maximum)),
            jnp.maximum(peak[1], fold(second, jnp.maximum)),
        )

    zero = jnp.zeros((8, cols), F32)
    found = chunks(rows, step, (zero, zero))
    lines = []
    for peak in found:
        peak = jnp.max(peak, axis=0, keepdims=True)
        lines += [peak[:, at : at + 128] for at in range(0, cols, 128)]
    lines = jnp.concatenate(lines, axis=0)
    for at in range(peaks.shape[0]):
        peaks[at] = lines


def clip(squares, grad, first_old, second_old, limit, group):
    rows, cols = grad.shape
    each = VMEM((rows, cols), F32)
    return call(
        functools.partial(clip_body, limit),
        (each, each, VMEM((group, 2 * cols // 128, 128), F32)),
        [],
        12 * rows * cols,
        20 * rows * cols,
        in_vmem(4),
    )(held(squares), grad, first_old, second_old)


def rows_body(first_new, second_new, direction, first_rowmax, second_rowmax, by_first, by_second):
    first, second = first_new[...], second_new[...]
    direction[0] = first / (jnp.sqrt(second) + epsilon)
    for values, least, peak, by in (
        (jnp.abs(first), scale_floor, first_rowmax, by_first),
        (second, 0.0, second_rowmax, by_second),
    ):
        tall = jnp.maximum(jnp.max(values, axis=1, keepdims=True), least)
        by[...] = jnp.broadcast_to(1.0 / tall, by.shape)
        peak[...] = row_of(tall)


def row_outputs(first_new, second_new):
    rows, cols = first_new.shape
    step = min(rows, 128)
    whole = pl.BlockSpec((step, cols), lambda r: (r, 0))
    side, line = pl.BlockSpec((step, 128), lambda r: (r, 0)), pl.BlockSpec((1, step), lambda r: (0, r))
    return pl.pallas_call(
        rows_body,
        grid=(rows // step,),
        out_shape=(
            jax.ShapeDtypeStruct((1, rows, cols), F32),
            jax.ShapeDtypeStruct((1, rows), F32),
            jax.ShapeDtypeStruct((1, rows), F32),
            VMEM((rows, 128), F32),
            VMEM((rows, 128), F32),
        ),
        in_specs=[whole, whole],
        out_specs=(pl.BlockSpec((1, step, cols), lambda r: (0, r, 0)), line, line, side, side),
        compiler_params=pltpu.CompilerParams(vmem_limit_bytes=VMEM_LIMIT),
        cost_estimate=pl.CostEstimate(flops=40 * rows * cols, bytes_accessed=12 * rows * cols, transcendentals=0),
        name="row_outputs",
    )(first_new, second_new)


def scaled_body(peaks, first_new, second_new, by_first, by_second, *refs):
    first_scaled, second_scaled, first_colmax, second_colmax, inverse = refs
    half = peaks.shape[1] // 2

    @pl.when(pl.program_id(0) == 0)
    def _():
        found = jnp.max(peaks[...], axis=0)
        for k, (out, least) in enumerate(((first_colmax, scale_floor), (second_colmax, 0.0))):
            wide = [found[k * half + at : k * half + at + 1] for at in range(half)]
            wide = jnp.maximum(jnp.concatenate(wide, axis=1), least)
            out[...] = wide
            inverse[k : k + 1, :] = 1.0 / wide

    step = first_scaled.shape[1]
    rows = pl.ds(pl.multiple_of(pl.program_id(0) * step, step), step)
    for k, (values, by, out) in enumerate(
        ((first_new, by_first, first_scaled), (second_new, by_second, second_scaled))
    ):
        out[0] = values[rows, :] * jnp.maximum(by[rows, 0:1], inverse[k : k + 1, :])


def scaled_outputs(peaks, first_new, second_new, by_first, by_second):
    rows, cols = first_new.shape
    step = min(rows, 64)
    out, line = pl.BlockSpec((1, step, cols), lambda r: (0, r, 0)), pl.BlockSpec((1, cols), lambda r: (0, 0))
    big, wide = jax.ShapeDtypeStruct((1, rows, cols), F32), jax.ShapeDtypeStruct((1, cols), F32)
    return pl.pallas_call(
        scaled_body,
        grid=(rows // step,),
        out_shape=(big, big, wide, wide),
        in_specs=in_vmem(5),
        out_specs=(out, out, line, line),
        scratch_shapes=[VMEM((8, cols), F32)],
        compiler_params=pltpu.CompilerParams(vmem_limit_bytes=VMEM_LIMIT),
        cost_estimate=pl.CostEstimate(flops=8 * rows * cols, bytes_accessed=16 * rows * cols, transcendentals=0),
        name="scaled_outputs",
    )(held(peaks), first_new, second_new, by_first, by_second)


def exchange(value, axes):
    return lax.all_to_all(value, axes, split_axis=0, concat_axis=0, tiled=True)


def local(
    grad_parts, first_codes, first_rows, first_columns, second_codes, second_rows, second_columns
):
    layer_count, _, row_count, col_count = grad_parts.shape
    entries = layer_count * lax.axis_size("section") * row_count * col_count
    devices, group = lax.axis_size(AXES), lax.axis_size(FSDP)
    parts = grad_parts.reshape(RING * RING, 2, 2, -1, col_count)
    old = (first_codes, first_rows, first_columns, second_codes, second_rows, second_columns)
    gradient, squares = reduce_scatter(parts, devices)
    first_old, second_old = old_moments(old)
    squares = exchange(squares, AXES)
    clip_limit = clip_rms * math.sqrt(entries)
    first_new, second_new, peaks = clip(squares, gradient, first_old, second_old, clip_limit, group)
    peaks = exchange(peaks, FSDP)
    direction, first_rowmax, second_rowmax, by_first, by_second = row_outputs(first_new, second_new)
    first_scaled, second_scaled, first_colmax, second_colmax = scaled_outputs(
        peaks, first_new, second_new, by_first, by_second
    )
    return (
        direction,
        first_scaled,
        second_scaled,
        first_rowmax,
        first_colmax,
        second_rowmax,
        second_colmax,
    )


def solution(mesh):
    torus = Mesh(mesh.devices.reshape(mesh.shape["section"], RING, RING, 2), AXES)
    placed = (
        P("section", FSDP, None, None),
        P("section", FSDP, None),
        P("section", FSDP),
        P("section", None),
        P("section", FSDP, None),
        P("section", FSDP),
        P("section", None),
    )
    return jax.shard_map(
        local,
        mesh=torus,
        in_specs=placed,
        out_specs=(
            P("section", FSDP, None),
            P("section", FSDP, None),
            P("section", FSDP, None),
            P("section", FSDP),
            P("section", None),
            P("section", FSDP),
            P("section", None),
        ),
        check_vma=False,
    )
```
